32 devices in a mesh: dp: 4 (over y, x), tp: 8 (over z, core).
Axes of the slice: x: 2, y: 2, z: 4, core: 2. Of those that a mesh axis runs over, the one named last changes fastest.
Arguments:
- proj_in: bfloat16 [1, 4096, 8192], P(None, 'dp', 'tp'), may hold values from -6 to 6
- kv_grad: bfloat16 [1, 4096, 2048], P(None, ('dp', 'tp')), may hold values from -0.1796875 to 0.1796875
- normed: bfloat16 [1, 4096, 8192], P(None, ('dp', 'tp')), may hold values from -6 to 6
- norm_grad: bfloat16 [1, 4096, 8192], P(None, ('dp', 'tp')), may hold values from -0.6 to 0.6
- first_moment: float32 [1, 8192, 2048], P(None, 'tp', 'dp'), may hold values from -0.6 to 0.6
- second_moment: float32 [1, 8192, 2048], P(None, 'tp', 'dp'), may hold values from 0.002 to 0.02
Outputs:
- new_first: float32 [1, 8192, 2048], P(None, 'tp', 'dp')
- new_second: float32 [1, 8192, 2048], P(None, 'tp', 'dp')
- adam_step: float32 [1, 8192, 2048], P(None, 'tp', 'dp')
- gain_grad: float32 [1, 8192], replicated
The draws below stay inside these ranges and needn't reach their ends.
All inputs are finite; a program needn't handle non-finite values.
Results may differ from the reference program's by a relative error of at most 0.0003.
Values may be sent and summed in bfloat16 or wider, within the bound.
A program may use at most 128 MiB of HBM per device.

```python
import math
import jax
import jax.numpy as jnp
from jax import lax

D = 8192
KV = 2048
LAYERS = 1
TOK_REP = 1024
TOKENS = 4096
N_DP = 4


def draw_norm_grad(key, part):
    first_key, second_key, third_key = jax.random.split(key, 3)
    values = 0.1 * jax.random.normal(first_key, (LAYERS, TOKENS, D), jnp.float32)
    return jnp.clip(values, -0.6, 0.6).astype(jnp.bfloat16)


def strengthened(result, own_key, source, target, parts, factor):
    def block_of(position):
        return (jnp.arange(result.shape[position]) // (result.shape[position] // parts)).reshape((-1,) + (1,) * (result.ndim - 1 - position))

    one_side = jax.random.permutation(own_key, parts)[block_of(target)]
    second = (block_of(target) + parts // 2) % parts
    return jnp.where((block_of(source) == one_side) | (block_of(source) == second), factor * result, result)


def block_levels(stream_key, dims, shards, least, top_value):
    factor_of, own = 1.0, jax.random.fold_in(stream_key, 6)
    for axis_at, parts in shards:
        draws = jnp.exp(jax.random.uniform(jax.random.fold_in(own, axis_at), (parts,), jnp.float32, least / len(shards), top_value / len(shards)))
        factor_of = factor_of * jnp.repeat(draws, dims[axis_at] // parts).reshape([-1 if axis == axis_at else 1 for axis in range(len(dims))])
    return factor_of


def bell_draw(rng, extent, scale, bound, pieces=(), held_as=jnp.bfloat16):
    loudness = block_levels(rng, extent, pieces, -0.22, 0.18) if pieces else 1.0
    array = jax.random.normal(rng, extent, jnp.float32) * scale * loudness
    return jnp.minimum(jnp.maximum(array, -bound), bound).astype(held_as)


def heavy_noise(key, shape, deviation, limit, cuts, heavy, held_as=jnp.bfloat16):
    drawn = deviation * jax.random.normal(key, shape, jnp.float32)
    if cuts:
        drawn = drawn * block_levels(key, shape, cuts, -0.22, 0.18)
    return jnp.clip(strengthened(drawn, jax.random.fold_in(key, 3), *heavy), -limit, limit).astype(held_as)


def setup_inputs(seed: int = 0) -> dict:
    splits = jax.random.split(jax.random.key(seed), 7)
    return {
        "proj_in": bell_draw(splits[0], (LAYERS, TOKENS, D), 1.0, 6.0, ((1, 4), (2, 8))),
        "kv_grad": heavy_noise(splits[1], (LAYERS, TOKENS, KV), 0.03, 0.1796875, ((1, 32),), (1, 2, 32, 2.75)),
        "normed": bell_draw(splits[2], (LAYERS, TOKENS, D), 1.0, 6.0, ((1, 32),)),
        "norm_grad": draw_norm_grad(jax.random.fold_in(splits[6], 71), 0),
        "first_moment": bell_draw(splits[4], (LAYERS, D, KV), 0.1, 0.6, ((1, 8), (2, 4)), jnp.float32),
        "second_moment": jnp.clip(jnp.exp(math.log(0.02) - 2.30258502 * jax.random.uniform(splits[5], (LAYERS, D, KV), jnp.float32) ** block_levels(splits[5], (LAYERS, D, KV), ((1, 8), (2, 4)), -0.2, 0.2)), 0.002, 0.02),
    }


beta_one = 0.9
beta_two = 0.95
correct_one = 0.19
correct_two = 0.0975
epsilon = 1e-08

def reference(proj_in, kv_grad, normed, norm_grad, first_moment, second_moment):
    firsts = []
    seconds = []
    updates = []
    for layer_id in range(LAYERS):
        running = jnp.zeros((D, KV), jnp.float32)
        for replica in range(N_DP):
            inputs = proj_in[layer_id, replica * TOK_REP:(replica + 1) * TOK_REP]
            grad_rows = kv_grad[layer_id, replica * TOK_REP:(replica + 1) * TOK_REP]
            product = lax.dot_general(inputs, grad_rows, (((0,), (0,)), ((), ())), preferred_element_type=jnp.float32)
            running = running + product
        mean_grad = running / N_DP
        new_first = beta_one * first_moment[layer_id] + (1.0 - beta_one) * mean_grad
        new_second = beta_two * second_moment[layer_id] + (1.0 - beta_two) * mean_grad * mean_grad
        update = new_first / correct_one / (jnp.sqrt(new_second / correct_two) + epsilon)
        firsts.append(new_first)
        seconds.append(new_second)
        updates.append(update)
    gain_grad = lax.optimization_barrier(jnp.sum(norm_grad.astype(jnp.float32) * normed.astype(jnp.float32), axis=1)) / N_DP
    return (jnp.stack(firsts), jnp.stack(seconds), jnp.stack(updates), gain_grad)
```

```python
import functools
import math

import jax
import jax.numpy as jnp
from jax import lax
from jax.experimental import pallas as pl
from jax.experimental.pallas import tpu as pltpu
from jax.sharding import PartitionSpec as P

beta_one = 0.9
beta_two = 0.95
correct_one = 0.19
correct_two = 0.0975
epsilon = 1e-08
PIECES = 4
LANES = 128
SPAN = 250.0
KNEE = 2.0 ** -5
VMEM_LIMIT = 46 * 1024 * 1024


def adam_update(mean_grad, first_old, second_old):
    new_first = beta_one * first_old + (1.0 - beta_one) * mean_grad
    new_second = beta_two * second_old + (1.0 - beta_two) * mean_grad * mean_grad
    update = new_first / correct_one / (jnp.sqrt(new_second / correct_two) + epsilon)
    return (new_first, new_second, update)


def kernel(
    n_dp, n_tp, x_hbm, g_hbm, a_hbm, b_hbm, sum_ref, gain_ref,
    xs, kv, a_buf, b_buf, gain_tp, gain_dp,
    local_sem, x_send, x_recv, a2a_send, a2a_recv,
    up_send, up_recv, down_send, down_recv, pair_send, pair_recv,
    gt_send, gt_recv, gd_send, gd_recv,
):
    dp = lax.axis_index("dp")
    tp = lax.axis_index("tp")
    z = tp // 2
    core = tp % 2
    n_z = n_tp // 2
    rows = g_hbm.shape[0]
    cols = kv.shape[2]
    tokens = x_hbm.shape[0]
    piece = tokens // PIECES

    def dp_peer(o):
        return jnp.bitwise_xor(dp, o)

    def tp_peer(o):
        return lax.rem(tp + o, n_tp)

    locals_ = [
        pltpu.make_async_copy(a_hbm, a_buf, local_sem.at[0]),
        pltpu.make_async_copy(b_hbm, b_buf, local_sem.at[1]),
        pltpu.make_async_copy(
            g_hbm.at[:, pl.ds(pl.multiple_of(dp * cols, cols), cols)],
            kv.at[dp, pl.ds(pl.multiple_of(tp * rows, rows), rows), :],
            local_sem.at[2],
        ),
        pltpu.make_async_copy(x_hbm, xs.at[dp], local_sem.at[3]),
    ]
    for copy in locals_:
        copy.start()

    barrier = pltpu.get_barrier_semaphore()
    for o in range(1, n_dp):
        pl.semaphore_signal(barrier, inc=1, device_id={"dp": dp_peer(o)}, device_id_type=pl.DeviceIdType.MESH)
    for o in range(1, n_tp):
        pl.semaphore_signal(barrier, inc=1, device_id={"tp": tp_peer(o)}, device_id_type=pl.DeviceIdType.MESH)
    pl.semaphore_wait(barrier, n_dp - 1 + n_tp - 1)

    sent = []

    def remote(src, dst, send, recv, where):
        return pltpu.make_async_remote_copy(
            src_ref=src, dst_ref=dst, send_sem=send, recv_sem=recv,
            device_id=where, device_id_type=pl.DeviceIdType.MESH,
        )

    my_rows = pl.ds(pl.multiple_of(tp * rows, rows), rows)
    a2a = []
    for o in range(1, n_dp):
        peer = dp_peer(o)
        copy = remote(
            g_hbm.at[:, pl.ds(pl.multiple_of(peer * cols, cols), cols)],
            kv.at[dp, my_rows, :], a2a_send.at[o], a2a_recv.at[o], {"dp": peer},
        )
        copy.start()
        a2a.append(copy)
        sent.append(copy)

    def x_copy(src, origin, c, o_recv, o_to, send):
        part = pl.ds(c * piece, piece)
        return remote(
            src.at[part, :], xs.at[origin, part, :], send, x_recv.at[o_recv, c],
            {"dp": dp_peer(o_to)},
        )

    square = n_dp == 4
    orders = {o: list(range(PIECES)) for o in range(1, n_dp)}
    half = PIECES // 2
    if square:
        orders[2] = list(range(half, PIECES)) + list(range(half))
        orders[3] = []

    def send_own(i):
        for o in range(1, n_dp):
            if i < len(orders[o]):
                c = orders[o][i]
                copy = x_copy(x_hbm, dp, c, o, o, x_send.at[o, c])
                copy.start()
                sent.append(copy)

    def got(o, c):
        x_copy(xs.at[dp_peer(o)], dp_peer(o), c, o, o, x_send.at[o, c]).wait_recv()

    def forward(i):
        for o, o_to in ((1, 2), (2, 1)):
            c = orders[o][i]
            got(o, c)
            copy = x_copy(xs.at[dp_peer(o)], dp_peer(o), c, 3, o_to, x_send.at[3, c])
            copy.start()
            sent.append(copy)

    send_own(0)
    send_own(1)

    locals_[0].wait()
    locals_[1].wait()
    wide = gain_tp.shape[2]
    lines = gain_tp.shape[1]
    for j in range(lines):
        s = pl.ds(j * wide, wide)
        products = a_buf[:, s].astype(jnp.float32) * b_buf[:, s].astype(jnp.float32)
        gain_tp[tp, pl.ds(j, 1), :] = jnp.sum(products, axis=0, keepdims=True)
    tp_copies = []
    for o in range(1, n_tp):
        copy = remote(gain_tp.at[tp], gain_tp.at[tp], gt_send.at[o], gt_recv.at[o], {"tp": tp_peer(o)})
        copy.start()
        sent.append(copy)
        tp_copies.append(copy)

    def block(b, c):
        return kv.at[:, pl.ds(pl.multiple_of((2 * b + c) * rows, rows), rows), :]

    other = 2 * z + 1 - core

    def to_pair(b):
        return remote(block(b, core), block(b, core), pair_send.at[b], pair_recv.at[b], {"tp": other})

    def up(s):
        b = z - s + 1
        return remote(block(b, core), block(b, core), up_send.at[s], up_recv.at[s], {"tp": tp + 2})

    def down(s):
        b = z + s - 1
        return remote(block(b, core), block(b, core), down_send.at[s], down_recv.at[s], {"tp": tp - 2})

    def up_got(s):
        b = z - s
        return remote(block(b, core), block(b, core), up_send.at[s], up_recv.at[s], {"tp": other})

    def down_got(s):
        b = z + s
        return remote(block(b, core), block(b, core), down_send.at[s], down_recv.at[s], {"tp": other})

    locals_[2].wait()
    for o in range(1, n_dp):
        a2a[o - 1].wait_recv()

    for s in range(1, n_z + 1):
        if s > 1:
            @pl.when(z - s + 1 >= 0)
            def _():
                up_got(s - 1).wait_recv()

        if s < n_z:
            @pl.when((z - s + 1 >= 0) & (z + 1 < n_z))
            def _():
                up(s).start()

        if s > 1:
            @pl.when(z + s - 1 < n_z)
            def _():
                down_got(s - 1).wait_recv()

        if s < n_z:
            @pl.when((z + s - 1 < n_z) & (z - 1 >= 0))
            def _():
                down(s).start()

        if s == 1:
            to_pair(z).start()
        else:
            @pl.when(z - s + 1 >= 0)
            def _():
                to_pair(z - s + 1).start()

            @pl.when(z + s - 1 < n_z)
            def _():
                to_pair(z + s - 1).start()

        if s == 1:
            for copy in tp_copies:
                copy.wait_recv()
            gain_dp[dp, :, :] = jnp.sum(gain_tp[...], axis=0)
            for o in range(1, n_dp):
                copy = remote(gain_dp.at[dp], gain_dp.at[dp], gd_send.at[o], gd_recv.at[o], {"dp": dp_peer(o)})
                copy.start()
                sent.append(copy)
            for i in range(2, PIECES):
                send_own(i)
        if square and 2 <= s < 2 + half:
            forward(s - 2)
    if square:
        for i in range(max(n_z - 1, 0), half):
            forward(i)

    for b in range(n_z):
        remote(block(b, 1 - core), block(b, 1 - core), pair_send.at[b], pair_recv.at[b], {"tp": other}).wait_recv()

    width = min(256, sum_ref.shape[0])

    def multiply(origin, start, size, first=False):
        @pl.loop(0, sum_ref.shape[0] // width)
        def _(f):
            at = pl.ds(pl.multiple_of(f * width, width), width)
            part = lax.dot_general(
                xs[origin, pl.ds(start, size), at], kv[origin, pl.ds(start, size), :],
                (((0,), (0,)), ((), ())), preferred_element_type=jnp.float32,
            )
            if first:
                sum_ref[at, :] = part
            else:
                sum_ref[at, :] += part

    locals_[3].wait()
    multiply(dp, 0, tokens, True)
    for o in range(1, n_dp):
        if square and o == 3:
            continue
        for c in orders[o]:
            if not (square and c in orders[o][:half]):
                got(o, c)
        multiply(dp_peer(o), 0, tokens)

    for o in range(1, n_dp):
        remote(gain_dp.at[dp_peer(o)], gain_dp.at[dp_peer(o)], gd_send.at[o], gd_recv.at[o], {"dp": dp_peer(o)}).wait_recv()
    gain_ref[...] = jnp.sum(gain_dp[...], axis=0) / n_dp

    if square:
        for i in range(half):
            for o in (1, 2):
                c = orders[o][i]
                got(3, c)
                multiply(dp_peer(3), c * piece, piece)

    for copy in sent:
        copy.wait_send()
    for s in range(1, n_z):
        @pl.when((z - s + 1 >= 0) & (z + 1 < n_z))
        def _():
            up(s).wait_send()

        @pl.when((z + s - 1 < n_z) & (z - 1 >= 0))
        def _():
            down(s).wait_send()
    for b in range(n_z):
        to_pair(b).wait_send()


def encode(value, bound):
    power = SPAN / math.log2(1.0 + bound / KNEE)
    code = jnp.exp2(power * jnp.log2(1.0 + jnp.abs(value) * (1.0 / KNEE)) - SPAN / 2)
    return jnp.where(value < 0.0, -code, code).astype(jnp.bfloat16)


def decode(code, bound):
    power = SPAN / math.log2(1.0 + bound / KNEE)
    code = code.astype(jnp.float32)
    value = (jnp.exp2((jnp.log2(jnp.abs(code)) + SPAN / 2) * (1.0 / power)) - 1.0) * KNEE
    return jnp.where(code < 0.0, -value, value)


def pair_kernel(
    n_tp, x_hbm, g_hbm, a_hbm, b_hbm, m_hbm, v_hbm, first_ref, second_ref, step_ref, gain_ref,
    xs, kv, part, arrived, own, m_buf, v_buf, a_buf, b_buf, gain_half, gain_pair, gain_x, gain_y, gain_z, gain_all,
    local_sem, swap_send, swap_recv, x_send, x_recv, part_send, part_recv,
    up_send, up_recv, down_send, down_recv, pair_send, pair_recv, gain_send, gain_recv,
):
    n_dp = 4
    dp = lax.axis_index("dp")
    tp = lax.axis_index("tp")
    z = tp // 2
    core = tp % 2
    n_z = n_tp // 2
    rows = g_hbm.shape[0]
    cols = kv.shape[2]
    tokens, features = x_hbm.shape
    chunks = features // LANES
    bound = 2.0 * tokens * 6.0 * 0.75
    other = 2 * z + 1 - core
    beside = jnp.bitwise_xor(dp, 1)
    across = jnp.bitwise_xor(dp, 2)
    sent = []

    def remote(src, dst, send, recv, where):
        return pltpu.make_async_remote_copy(
            src_ref=src, dst_ref=dst, send_sem=send, recv_sem=recv,
            device_id=where, device_id_type=pl.DeviceIdType.MESH,
        )

    def go(copy):
        copy.start()
        sent.append(copy)

    my_rows = pl.ds(pl.multiple_of(tp * rows, rows), rows)

    def g_cols(d):
        return g_hbm.at[:, pl.ds(pl.multiple_of(d * cols, cols), cols)]

    locals_ = [
        pltpu.make_async_copy(g_cols(across), kv.at[0, my_rows, :], local_sem.at[0]),
        pltpu.make_async_copy(g_cols(dp), kv.at[2, my_rows, :], local_sem.at[1]),
        pltpu.make_async_copy(a_hbm, a_buf, local_sem.at[2]),
        pltpu.make_async_copy(b_hbm, b_buf, local_sem.at[3]),
        pltpu.make_async_copy(x_hbm, xs.at[0], local_sem.at[4]),
        pltpu.make_async_copy(m_hbm, m_buf, local_sem.at[5]),
        pltpu.make_async_copy(v_hbm, v_buf, local_sem.at[6]),
    ]
    for copy in locals_:
        copy.start()

    barrier = pltpu.get_barrier_semaphore()

    def hello(where):
        pl.semaphore_signal(barrier, inc=1, device_id=where, device_id_type=pl.DeviceIdType.MESH)

    hello({"dp": beside})
    hello({"dp": across})
    hello({"tp": other})

    @pl.when(z + 1 < n_z)
    def _():
        hello({"tp": tp + 2})

    @pl.when(z >= 1)
    def _():
        hello({"tp": tp - 2})

    pl.semaphore_wait(barrier, 3 + jnp.where(z + 1 < n_z, 1, 0) + jnp.where(z >= 1, 1, 0))

    def swap(i, plane, d):
        return remote(g_cols(d), kv.at[plane, my_rows, :], swap_send.at[i], swap_recv.at[i], {"dp": beside})

    swaps = [swap(0, 1, jnp.bitwise_xor(dp, 3)), swap(1, 3, beside)]

    def x_copy(k):
        at = pl.ds(k * LANES, LANES)
        return remote(x_hbm.at[:, at], xs.at[1, :, at], x_send.at[k], x_recv.at[k], {"dp": beside})

    go(swaps[0])
    go(swaps[1])
    for k in range(chunks):
        go(x_copy(k))

    GAIN = 4

    def block(g, b, c):
        if g == GAIN:
            return gain_z.at[b]
        return kv.at[g, pl.ds(pl.multiple_of((2 * b + c) * rows, rows), rows), :]

    def to_pair(g, b):
        return remote(block(g, b, core), block(g, b, core), pair_send.at[g, b], pair_recv.at[g, b], {"tp": other})

    def from_pair(g, b):
        return remote(block(g, b, 1 - core), block(g, b, 1 - core), pair_send.at[g, b], pair_recv.at[g, b], {"tp": other})

    def up(g, s):
        b = z - s + 1
        return remote(block(g, b, core), block(g, b, core), up_send.at[g, s], up_recv.at[g, s], {"tp": tp + 2})

    def down(g, s):
        b = z + s - 1
        return remote(block(g, b, core), block(g, b, core), down_send.at[g, s], down_recv.at[g, s], {"tp": tp - 2})

    def up_got(g, s):
        b = z - s
        return remote(block(g, b, core), block(g, b, core), up_send.at[g, s], up_recv.at[g, s], {"tp": other})

    def down_got(g, s):
        b = z + s
        return remote(block(g, b, core), block(g, b, core), down_send.at[g, s], down_recv.at[g, s], {"tp": other})

    def chain(g, s):
        if s > 1:
            @pl.when(z - s + 1 >= 0)
            def _():
                up_got(g, s - 1).wait_recv()

        if s < n_z:
            @pl.when((z - s + 1 >= 0) & (z + 1 < n_z))
            def _():
                up(g, s).start()

        if s > 1:
            @pl.when(z + s - 1 < n_z)
            def _():
                down_got(g, s - 1).wait_recv()

        if s < n_z:
            @pl.when((z + s - 1 < n_z) & (z - 1 >= 0))
            def _():
                down(g, s).start()

        if g == GAIN:
            return
        if s == 1:
            to_pair(g, z).start()
        else:
            @pl.when(z - s + 1 >= 0)
            def _():
                to_pair(g, z - s + 1).start()

            @pl.when(z + s - 1 < n_z)
            def _():
                to_pair(g, z + s - 1).start()

    def complete(g):
        for b in range(n_z):
            from_pair(g, b).wait_recv()

    def gain_copy(i, src, dst, where):
        return remote(src, dst, gain_send.at[i], gain_recv.at[i], where)

    def dot(x, w):
        return lax.dot_general(x, w, (((0,), (0,)), ((), ())), preferred_element_type=jnp.float32)

    halves = 2
    wide = cols // halves

    def part_copy(k, h):
        at = (pl.ds(k * LANES, LANES), pl.ds(h * wide, wide))
        return remote(part.at[at], arrived.at[at], part_send.at[k, h], part_recv.at[k, h], {"dp": across})

    def partial(k):
        at = pl.ds(k * LANES, LANES)
        x_copy(k).wait_recv()
        for h in range(halves):
            ch = pl.ds(h * wide, wide)
            total = dot(xs[0, :, at], kv[0, :, ch]) + dot(xs[1, :, at], kv[1, :, ch])
            part[at, ch] = encode(total, bound)
            go(part_copy(k, h))

    def own_sum(k):
        at = pl.ds(k * LANES, LANES)
        own[at, :] = dot(xs[0, :, at], kv[2]) + dot(xs[1, :, at], kv[3])

    def finish(k):
        at = pl.ds(k * LANES, LANES)
        for h in range(halves):
            ch = pl.ds(h * wide, wide)
            part_copy(k, h).wait_recv()
            mean = (own[at, ch] + decode(arrived[at, ch], bound)) / n_dp
            new_first, new_second, update = adam_update(mean, m_buf[at, ch], v_buf[at, ch])
            first_ref[at, ch] = new_first
            second_ref[at, ch] = new_second
            step_ref[at, ch] = update

    locals_[0].wait()
    chain(0, 1)
    locals_[1].wait()
    chain(2, 1)

    locals_[2].wait()
    locals_[3].wait()
    lines, span = gain_half.shape[1:]
    for h in range(2):
        for j in range(lines):
            at = pl.ds((h * lines + j) * span, span)
            products = a_buf[:, at].astype(jnp.float32) * b_buf[:, at].astype(jnp.float32)
            gain_half[h, pl.ds(j, 1), :] = jnp.sum(products, axis=0, keepdims=True)
    go(gain_copy(0, gain_half.at[1 - core], gain_pair.at[1], {"tp": other}))
    swaps[0].wait_recv()
    chain(1, 1)
    chain(0, 2)
    gain_copy(0, gain_half.at[1 - core], gain_pair.at[1], {"tp": other}).wait_recv()
    gain_x[0] = gain_half[core] + gain_pair[1]
    go(gain_copy(1, gain_x.at[0], gain_x.at[1], {"dp": beside}))
    chain(1, 2)
    chain(0, 3)
    chain(1, 3)
    swaps[1].wait_recv()
    chain(3, 1)
    chain(2, 2)
    for s in range(4, n_z + 1):
        chain(0, s)
        chain(1, s)
    complete(0)
    complete(1)
    locals_[4].wait()

    partial(0)
    gain_copy(1, gain_x.at[0], gain_x.at[1], {"dp": beside}).wait_recv()
    gain_y[0] = gain_x[0] + gain_x[1]
    go(gain_copy(2, gain_y.at[0], gain_y.at[1], {"dp": across}))
    chain(3, 2)
    chain(2, 3)
    partial(1)
    gain_copy(2, gain_y.at[0], gain_y.at[1], {"dp": across}).wait_recv()
    gain_z[z] = gain_y[0] + gain_y[1]
    chain(GAIN, 1)
    chain(3, 3)
    partial(2)
    chain(GAIN, 2)
    for s in range(4, n_z + 1):
        chain(2, s)
        chain(3, s)
    partial(3)
    for s in range(3, n_z + 1):
        chain(GAIN, s)
    complete(2)
    complete(3)
    own_sum(0)
    own_sum(1)
    gain_all[core] = jnp.sum(gain_z[...], axis=0) / n_dp
    go(gain_copy(3, gain_all.at[core], gain_all.at[core], {"tp": other}))
    for copy in locals_[5:]:
        copy.wait()
    finish(0)
    done, finished = 2, 1
    for k in range(4, chunks):
        partial(k)
        while done < k:
            own_sum(done)
            done += 1
            if finished < done - 1:
                finish(finished)
                finished += 1
        if k == 4:
            gain_copy(3, gain_all.at[1 - core], gain_all.at[1 - core], {"tp": other}).wait_recv()
            per = span // LANES
            for h in range(2):
                for i in range(per):
                    at = pl.ds(h * lines * per + i, lines, stride=per)
                    gain_ref[at, :] = gain_all[h, :, i * LANES:(i + 1) * LANES]
    while done < chunks:
        own_sum(done)
        done += 1
    while finished < chunks:
        finish(finished)
        finished += 1

    for copy in sent:
        copy.wait_send()
    for g in range(GAIN + 1):
        for s in range(1, n_z):
            @pl.when((z - s + 1 >= 0) & (z + 1 < n_z))
            def _():
                up(g, s).wait_send()

            @pl.when((z + s - 1 < n_z) & (z - 1 >= 0))
            def _():
                down(g, s).wait_send()
        if g < GAIN:
            for b in range(n_z):
                to_pair(g, b).wait_send()


def store_kernel(*refs):
    count = (len(refs) - 1) // 2
    copies = [pltpu.make_async_copy(refs[i], refs[count + i], refs[-1].at[i]) for i in range(count)]
    for copy in copies:
        copy.start()
    for copy in copies:
        copy.wait()


def store_call(*arrays):
    return pl.pallas_call(
        store_kernel,
        out_shape=tuple(jax.ShapeDtypeStruct(a.shape, a.dtype) for a in arrays),
        in_specs=[pl.BlockSpec(memory_space=pltpu.VMEM)] * len(arrays),
        out_specs=(pl.BlockSpec(memory_space=pltpu.HBM),) * len(arrays),
        scratch_shapes=[pltpu.SemaphoreType.DMA((len(arrays),))],
        compiler_params=pltpu.CompilerParams(vmem_limit_bytes=1024 * 1024),
    )(*arrays)


def pair_call(layer, n_tp, x, g, a, b, m, v):
    tokens, features = x.shape
    rows, width = g.shape
    model = a.shape[1]
    n_dp = 4
    cols = width // n_dp
    n_z = n_tp // 2
    chunks = features // LANES
    span = model // 16
    dma = pltpu.SemaphoreType.DMA
    bf16, f32 = jnp.bfloat16, jnp.float32
    buffers = [
        ((2, tokens, features), bf16), ((4, tokens, cols), bf16),
        ((features, cols), bf16), ((features, cols), bf16), ((features, cols), f32),
        ((features, cols), f32), ((features, cols), f32),
        ((rows, model), bf16), ((rows, model), bf16),
        ((2, 8, span), f32), ((2, 8, span), f32), ((2, 8, span), f32), ((2, 8, span), f32),
        ((n_z, 8, span), f32), ((2, 8, span), f32),
    ]
    total = jax.ShapeDtypeStruct((features, cols), f32)
    return pl.pallas_call(
        functools.partial(pair_kernel, n_tp),
        out_shape=(total, total, total, jax.ShapeDtypeStruct((model // LANES, LANES), f32)),
        in_specs=[pl.BlockSpec(memory_space=pltpu.HBM)] * 6,
        out_specs=(pl.BlockSpec(memory_space=pltpu.VMEM),) * 4,
        scratch_shapes=[pltpu.VMEM(shape, dtype) for shape, dtype in buffers] + [
            dma((7,)), dma((2,)), dma((2,)), dma((chunks,)), dma((chunks,)), dma((chunks, 2)), dma((chunks, 2)),
        ] + [dma((5, n_z))] * 6 + [dma((4,)), dma((4,))],
        compiler_params=pltpu.CompilerParams(
            collective_id=layer, has_side_effects=True, vmem_limit_bytes=VMEM_LIMIT,
        ),
    )(x, g, a, b, m, v)


def shards(n_dp, n_tp, proj_in, kv_grad, normed, norm_grad, first_moment, second_moment):
    layers, tokens, features = proj_in.shape
    rows, width = kv_grad.shape[1:]
    model = normed.shape[2]
    cols = width // n_dp
    lines = 8
    dma = pltpu.SemaphoreType.DMA
    n_z = n_tp // 2
    firsts, seconds, updates, gains = [], [], [], []
    for layer in range(layers):
        if n_dp == 4 and features % LANES == 0 and features >= 6 * LANES and model % (16 * LANES) == 0 and n_tp >= 6:
            new_first, new_second, update, gain = store_call(*pair_call(
                layer, n_tp, proj_in[layer], kv_grad[layer], normed[layer], norm_grad[layer],
                first_moment[layer], second_moment[layer],
            ))
        else:
            total, gain = pl.pallas_call(
                functools.partial(kernel, n_dp, n_tp),
                out_shape=(
                    jax.ShapeDtypeStruct((features, cols), jnp.float32),
                    jax.ShapeDtypeStruct((lines, model // lines), jnp.float32),
                ),
                in_specs=[pl.BlockSpec(memory_space=pltpu.HBM)] * 4,
                out_specs=(pl.BlockSpec(memory_space=pltpu.VMEM), pl.BlockSpec(memory_space=pltpu.VMEM)),
                scratch_shapes=[
                    pltpu.VMEM((n_dp, tokens, features), jnp.bfloat16),
                    pltpu.VMEM((n_dp, n_tp * rows, cols), jnp.bfloat16),
                    pltpu.VMEM((rows, model), jnp.bfloat16),
                    pltpu.VMEM((rows, model), jnp.bfloat16),
                    pltpu.VMEM((n_tp, lines, model // lines), jnp.float32),
                    pltpu.VMEM((n_dp, lines, model // lines), jnp.float32),
                    dma((4,)),
                    dma((n_dp, PIECES)), dma((n_dp, PIECES)),
                    dma((n_dp,)), dma((n_dp,)),
                    dma((n_z,)), dma((n_z,)), dma((n_z,)), dma((n_z,)),
                    dma((n_z,)), dma((n_z,)),
                    dma((n_tp,)), dma((n_tp,)), dma((n_dp,)), dma((n_dp,)),
                ],
                compiler_params=pltpu.CompilerParams(
                    collective_id=layer, has_side_effects=True, vmem_limit_bytes=60 * 1024 * 1024,
                ),
            )(proj_in[layer], kv_grad[layer], normed[layer], norm_grad[layer])
            new_first, new_second, update = adam_update(total / n_dp, first_moment[layer], second_moment[layer])
        firsts.append(new_first)
        seconds.append(new_second)
        updates.append(update)
        gains.append(gain.reshape(model))
    return (jnp.stack(firsts), jnp.stack(seconds), jnp.stack(updates), jnp.stack(gains))


def solution(mesh):
    return jax.shard_map(
        functools.partial(shards, mesh.shape["dp"], mesh.shape["tp"]),
        mesh=mesh,
        in_specs=(
            P(None, "dp", "tp"),
            P(None, ("dp", "tp"), None),
            P(None, ("dp", "tp"), None),
            P(None, ("dp", "tp"), None),
            P(None, "tp", "dp"),
            P(None, "tp", "dp"),
        ),
        out_specs=(P(None, "tp", "dp"), P(None, "tp", "dp"), P(None, "tp", "dp"), P()),
        check_vma=False,
    )
```

```python
import functools
import math

import jax
import jax.numpy as jnp
from jax import lax
from jax.experimental import pallas as pl
from jax.experimental.pallas import tpu as pltpu
from jax.sharding import PartitionSpec as P

beta_one = 0.9
beta_two = 0.95
correct_one = 0.19
correct_two = 0.0975
epsilon = 1e-08
PIECES = 4
LANES = 128
SPAN = 250.0
KNEE = 2.0 ** -5
EARLY = 2
VMEM_LIMIT = 46 * 1024 * 1024


def adam_update(mean_grad, first_old, second_old):
    new_first = beta_one * first_old + (1.0 - beta_one) * mean_grad
    new_second = beta_two * second_old + (1.0 - beta_two) * mean_grad * mean_grad
    update = new_first / correct_one / (jnp.sqrt(new_second / correct_two) + epsilon)
    return (new_first, new_second, update)


def kernel(
    n_dp, n_tp, x_hbm, g_hbm, a_hbm, b_hbm, sum_ref, gain_ref,
    xs, kv, a_buf, b_buf, gain_tp, gain_dp,
    local_sem, x_send, x_recv, a2a_send, a2a_recv,
    up_send, up_recv, down_send, down_recv, pair_send, pair_recv,
    gt_send, gt_recv, gd_send, gd_recv,
):
    dp = lax.axis_index("dp")
    tp = lax.axis_index("tp")
    z = tp // 2
    core = tp % 2
    n_z = n_tp // 2
    rows = g_hbm.shape[0]
    cols = kv.shape[2]
    tokens = x_hbm.shape[0]
    piece = tokens // PIECES

    def dp_peer(o):
        return jnp.bitwise_xor(dp, o)

    def tp_peer(o):
        return lax.rem(tp + o, n_tp)

    locals_ = [
        pltpu.make_async_copy(a_hbm, a_buf, local_sem.at[0]),
        pltpu.make_async_copy(b_hbm, b_buf, local_sem.at[1]),
        pltpu.make_async_copy(
            g_hbm.at[:, pl.ds(pl.multiple_of(dp * cols, cols), cols)],
            kv.at[dp, pl.ds(pl.multiple_of(tp * rows, rows), rows), :],
            local_sem.at[2],
        ),
        pltpu.make_async_copy(x_hbm, xs.at[dp], local_sem.at[3]),
    ]
    for copy in locals_:
        copy.start()

    barrier = pltpu.get_barrier_semaphore()
    for o in range(1, n_dp):
        pl.semaphore_signal(barrier, inc=1, device_id={"dp": dp_peer(o)}, device_id_type=pl.DeviceIdType.MESH)
    for o in range(1, n_tp):
        pl.semaphore_signal(barrier, inc=1, device_id={"tp": tp_peer(o)}, device_id_type=pl.DeviceIdType.MESH)
    pl.semaphore_wait(barrier, n_dp - 1 + n_tp - 1)

    sent = []

    def remote(src, dst, send, recv, where):
        return pltpu.make_async_remote_copy(
            src_ref=src, dst_ref=dst, send_sem=send, recv_sem=recv,
            device_id=where, device_id_type=pl.DeviceIdType.MESH,
        )

    my_rows = pl.ds(pl.multiple_of(tp * rows, rows), rows)
    a2a = []
    for o in range(1, n_dp):
        peer = dp_peer(o)
        copy = remote(
            g_hbm.at[:, pl.ds(pl.multiple_of(peer * cols, cols), cols)],
            kv.at[dp, my_rows, :], a2a_send.at[o], a2a_recv.at[o], {"dp": peer},
        )
        copy.start()
        a2a.append(copy)
        sent.append(copy)

    def x_copy(src, origin, c, o_recv, o_to, send):
        part = pl.ds(c * piece, piece)
        return remote(
            src.at[part, :], xs.at[origin, part, :], send, x_recv.at[o_recv, c],
            {"dp": dp_peer(o_to)},
        )

    square = n_dp == 4
    orders = {o: list(range(PIECES)) for o in range(1, n_dp)}
    half = PIECES // 2
    if square:
        orders[2] = list(range(half, PIECES)) + list(range(half))
        orders[3] = []

    def send_own(i):
        for o in range(1, n_dp):
            if i < len(orders[o]):
                c = orders[o][i]
                copy = x_copy(x_hbm, dp, c, o, o, x_send.at[o, c])
                copy.start()
                sent.append(copy)

    def got(o, c):
        x_copy(xs.at[dp_peer(o)], dp_peer(o), c, o, o, x_send.at[o, c]).wait_recv()

    def forward(i):
        for o, o_to in ((1, 2), (2, 1)):
            c = orders[o][i]
            got(o, c)
            copy = x_copy(xs.at[dp_peer(o)], dp_peer(o), c, 3, o_to, x_send.at[3, c])
            copy.start()
            sent.append(copy)

    send_own(0)
    send_own(1)

    locals_[0].wait()
    locals_[1].wait()
    wide = gain_tp.shape[2]
    lines = gain_tp.shape[1]
    for j in range(lines):
        s = pl.ds(j * wide, wide)
        products = a_buf[:, s].astype(jnp.float32) * b_buf[:, s].astype(jnp.float32)
        gain_tp[tp, pl.ds(j, 1), :] = jnp.sum(products, axis=0, keepdims=True)
    tp_copies = []
    for o in range(1, n_tp):
        copy = remote(gain_tp.at[tp], gain_tp.at[tp], gt_send.at[o], gt_recv.at[o], {"tp": tp_peer(o)})
        copy.start()
        sent.append(copy)
        tp_copies.append(copy)

    def block(b, c):
        return kv.at[:, pl.ds(pl.multiple_of((2 * b + c) * rows, rows), rows), :]

    other = 2 * z + 1 - core

    def to_pair(b):
        return remote(block(b, core), block(b, core), pair_send.at[b], pair_recv.at[b], {"tp": other})

    def up(s):
        b = z - s + 1
        return remote(block(b, core), block(b, core), up_send.at[s], up_recv.at[s], {"tp": tp + 2})

    def down(s):
        b = z + s - 1
        return remote(block(b, core), block(b, core), down_send.at[s], down_recv.at[s], {"tp": tp - 2})

    def up_got(s):
        b = z - s
        return remote(block(b, core), block(b, core), up_send.at[s], up_recv.at[s], {"tp": other})

    def down_got(s):
        b = z + s
        return remote(block(b, core), block(b, core), down_send.at[s], down_recv.at[s], {"tp": other})

    locals_[2].wait()
    for o in range(1, n_dp):
        a2a[o - 1].wait_recv()

    for s in range(1, n_z + 1):
        if s > 1:
            @pl.when(z - s + 1 >= 0)
            def _():
                up_got(s - 1).wait_recv()

        if s < n_z:
            @pl.when((z - s + 1 >= 0) & (z + 1 < n_z))
            def _():
                up(s).start()

        if s > 1:
            @pl.when(z + s - 1 < n_z)
            def _():
                down_got(s - 1).wait_recv()

        if s < n_z:
            @pl.when((z + s - 1 < n_z) & (z - 1 >= 0))
            def _():
                down(s).start()

        if s == 1:
            to_pair(z).start()
        else:
            @pl.when(z - s + 1 >= 0)
            def _():
                to_pair(z - s + 1).start()

            @pl.when(z + s - 1 < n_z)
            def _():
                to_pair(z + s - 1).start()

        if s == 1:
            for copy in tp_copies:
                copy.wait_recv()
            gain_dp[dp, :, :] = jnp.sum(gain_tp[...], axis=0)
            for o in range(1, n_dp):
                copy = remote(gain_dp.at[dp], gain_dp.at[dp], gd_send.at[o], gd_recv.at[o], {"dp": dp_peer(o)})
                copy.start()
                sent.append(copy)
            for i in range(2, PIECES):
                send_own(i)
        if square and 2 <= s < 2 + half:
            forward(s - 2)
    if square:
        for i in range(max(n_z - 1, 0), half):
            forward(i)

    for b in range(n_z):
        remote(block(b, 1 - core), block(b, 1 - core), pair_send.at[b], pair_recv.at[b], {"tp": other}).wait_recv()

    width = min(256, sum_ref.shape[0])

    def multiply(origin, start, size, first=False):
        @pl.loop(0, sum_ref.shape[0] // width)
        def _(f):
            at = pl.ds(pl.multiple_of(f * width, width), width)
            part = lax.dot_general(
                xs[origin, pl.ds(start, size), at], kv[origin, pl.ds(start, size), :],
                (((0,), (0,)), ((), ())), preferred_element_type=jnp.float32,
            )
            if first:
                sum_ref[at, :] = part
            else:
                sum_ref[at, :] += part

    locals_[3].wait()
    multiply(dp, 0, tokens, True)
    for o in range(1, n_dp):
        if square and o == 3:
            continue
        for c in orders[o]:
            if not (square and c in orders[o][:half]):
                got(o, c)
        multiply(dp_peer(o), 0, tokens)

    for o in range(1, n_dp):
        remote(gain_dp.at[dp_peer(o)], gain_dp.at[dp_peer(o)], gd_send.at[o], gd_recv.at[o], {"dp": dp_peer(o)}).wait_recv()
    gain_ref[...] = jnp.sum(gain_dp[...], axis=0) / n_dp

    if square:
        for i in range(half):
            for o in (1, 2):
                c = orders[o][i]
                got(3, c)
                multiply(dp_peer(3), c * piece, piece)

    for copy in sent:
        copy.wait_send()
    for s in range(1, n_z):
        @pl.when((z - s + 1 >= 0) & (z + 1 < n_z))
        def _():
            up(s).wait_send()

        @pl.when((z + s - 1 < n_z) & (z - 1 >= 0))
        def _():
            down(s).wait_send()
    for b in range(n_z):
        to_pair(b).wait_send()


def encode(value, bound):
    power = SPAN / math.log2(1.0 + bound / KNEE)
    code = jnp.exp2(power * jnp.log2(1.0 + jnp.abs(value) * (1.0 / KNEE)) - SPAN / 2)
    return jnp.where(value < 0.0, -code, code).astype(jnp.bfloat16)


def decode(code, bound):
    power = SPAN / math.log2(1.0 + bound / KNEE)
    code = code.astype(jnp.float32)
    value = (jnp.exp2((jnp.log2(jnp.abs(code)) + SPAN / 2) * (1.0 / power)) - 1.0) * KNEE
    return jnp.where(code < 0.0, -value, value)


def pair_kernel(
    n_tp, x_hbm, g_hbm, a_hbm, b_hbm, m_hbm, v_hbm, first_ref, second_ref, step_ref, gain_ref,
    xs, kv, part, arrived, own, m_buf, v_buf, a_buf, b_buf, gain_half, gain_pair, gain_x, gain_y, gain_z, gain_all,
    local_sem, swap_send, swap_recv, x_send, x_recv, part_send, part_recv,
    up_send, up_recv, down_send, down_recv, pair_send, pair_recv, gain_send, gain_recv,
):
    n_dp = 4
    dp = lax.axis_index("dp")
    tp = lax.axis_index("tp")
    z = tp // 2
    core = tp % 2
    n_z = n_tp // 2
    rows = g_hbm.shape[0]
    cols = kv.shape[2]
    tokens, features = x_hbm.shape
    chunks = features // LANES
    bound = 2.0 * tokens * 6.0 * 0.75
    other = 2 * z + 1 - core
    beside = jnp.bitwise_xor(dp, 1)
    across = jnp.bitwise_xor(dp, 2)
    sent = []

    def remote(src, dst, send, recv, where):
        return pltpu.make_async_remote_copy(
            src_ref=src, dst_ref=dst, send_sem=send, recv_sem=recv,
            device_id=where, device_id_type=pl.DeviceIdType.MESH,
        )

    def go(copy):
        copy.start()
        sent.append(copy)

    my_rows = pl.ds(pl.multiple_of(tp * rows, rows), rows)

    def g_cols(d):
        return g_hbm.at[:, pl.ds(pl.multiple_of(d * cols, cols), cols)]

    locals_ = [
        pltpu.make_async_copy(g_cols(across), kv.at[0, my_rows, :], local_sem.at[0]),
        pltpu.make_async_copy(g_cols(dp), kv.at[2, my_rows, :], local_sem.at[1]),
        pltpu.make_async_copy(a_hbm, a_buf, local_sem.at[2]),
        pltpu.make_async_copy(b_hbm, b_buf, local_sem.at[3]),
        pltpu.make_async_copy(x_hbm, xs.at[0], local_sem.at[4]),
        pltpu.make_async_copy(m_hbm, m_buf, local_sem.at[5]),
        pltpu.make_async_copy(v_hbm, v_buf, local_sem.at[6]),
    ]
    for copy in locals_:
        copy.start()

    barrier = pltpu.get_barrier_semaphore()

    def hello(where):
        pl.semaphore_signal(barrier, inc=1, device_id=where, device_id_type=pl.DeviceIdType.MESH)

    hello({"dp": beside})
    hello({"dp": across})
    hello({"tp": other})

    @pl.when(z + 1 < n_z)
    def _():
        hello({"tp": tp + 2})

    @pl.when(z >= 1)
    def _():
        hello({"tp": tp - 2})

    pl.semaphore_wait(barrier, 3 + jnp.where(z + 1 < n_z, 1, 0) + jnp.where(z >= 1, 1, 0))

    def swap(i, plane, d):
        return remote(g_cols(d), kv.at[plane, my_rows, :], swap_send.at[i], swap_recv.at[i], {"dp": beside})

    swaps = [swap(0, 1, jnp.bitwise_xor(dp, 3)), swap(1, 3, beside)]

    def x_copy(k):
        at = pl.ds(k * LANES, LANES)
        return remote(x_hbm.at[:, at], xs.at[1, :, at], x_send.at[k], x_recv.at[k], {"dp": beside})

    go(swaps[0])
    go(swaps[1])
    for k in range(EARLY):
        go(x_copy(k))

    GAIN = 4

    def block(g, b, c):
        if g == GAIN:
            return gain_z.at[b]
        return kv.at[g, pl.ds(pl.multiple_of((2 * b + c) * rows, rows), rows), :]

    def to_pair(g, b):
        return remote(block(g, b, core), block(g, b, core), pair_send.at[g, b], pair_recv.at[g, b], {"tp": other})

    def from_pair(g, b):
        return remote(block(g, b, 1 - core), block(g, b, 1 - core), pair_send.at[g, b], pair_recv.at[g, b], {"tp": other})

    def up(g, s):
        b = z - s + 1
        return remote(block(g, b, core), block(g, b, core), up_send.at[g, s], up_recv.at[g, s], {"tp": tp + 2})

    def down(g, s):
        b = z + s - 1
        return remote(block(g, b, core), block(g, b, core), down_send.at[g, s], down_recv.at[g, s], {"tp": tp - 2})

    def up_got(g, s):
        b = z - s
        return remote(block(g, b, core), block(g, b, core), up_send.at[g, s], up_recv.at[g, s], {"tp": other})

    def down_got(g, s):
        b = z + s
        return remote(block(g, b, core), block(g, b, core), down_send.at[g, s], down_recv.at[g, s], {"tp": other})

    def chain(g, s):
        if s > 1:
            @pl.when(z - s + 1 >= 0)
            def _():
                up_got(g, s - 1).wait_recv()

        if s < n_z:
            @pl.when((z - s + 1 >= 0) & (z + 1 < n_z))
            def _():
                up(g, s).start()

        if s > 1:
            @pl.when(z + s - 1 < n_z)
            def _():
                down_got(g, s - 1).wait_recv()

        if s < n_z:
            @pl.when((z + s - 1 < n_z) & (z - 1 >= 0))
            def _():
                down(g, s).start()

        if g == GAIN:
            return
        if s == 1:
            to_pair(g, z).start()
        else:
            @pl.when(z - s + 1 >= 0)
            def _():
                to_pair(g, z - s + 1).start()

            @pl.when(z + s - 1 < n_z)
            def _():
                to_pair(g, z + s - 1).start()

    def complete(g):
        for b in range(n_z):
            from_pair(g, b).wait_recv()

    def gain_copy(i, src, dst, where):
        return remote(src, dst, gain_send.at[i], gain_recv.at[i], where)

    def dot(x, w):
        return lax.dot_general(x, w, (((0,), (0,)), ((), ())), preferred_element_type=jnp.float32)

    halves = 2
    wide = cols // halves

    def part_copy(k, h):
        at = (pl.ds(k * LANES, LANES), pl.ds(h * wide, wide))
        return remote(part.at[at], arrived.at[at], part_send.at[k, h], part_recv.at[k, h], {"dp": across})

    def partial(k):
        at = pl.ds(k * LANES, LANES)
        x_copy(k).wait_recv()
        for h in range(halves):
            ch = pl.ds(h * wide, wide)
            total = dot(xs[0, :, at], kv[0, :, ch]) + dot(xs[1, :, at], kv[1, :, ch])
            part[at, ch] = encode(total, bound)
            go(part_copy(k, h))

    def own_sum(k):
        at = pl.ds(k * LANES, LANES)
        own[at, :] = dot(xs[0, :, at], kv[2]) + dot(xs[1, :, at], kv[3])

    def finish(k):
        at = pl.ds(k * LANES, LANES)
        for h in range(halves):
            ch = pl.ds(h * wide, wide)
            part_copy(k, h).wait_recv()
            mean = (own[at, ch] + decode(arrived[at, ch], bound)) / n_dp
            new_first, new_second, update = adam_update(mean, m_buf[at, ch], v_buf[at, ch])
            first_ref[at, ch] = new_first
            second_ref[at, ch] = new_second
            step_ref[at, ch] = update

    locals_[0].wait()
    chain(0, 1)
    locals_[1].wait()
    chain(2, 1)

    locals_[2].wait()
    locals_[3].wait()
    lines, span = gain_half.shape[1:]
    for h in range(2):
        for j in range(lines):
            at = pl.ds((h * lines + j) * span, span)
            products = a_buf[:, at].astype(jnp.float32) * b_buf[:, at].astype(jnp.float32)
            gain_half[h, pl.ds(j, 1), :] = jnp.sum(products, axis=0, keepdims=True)
    pair_gain = gain_copy(0, gain_half.at[1 - core], gain_pair.at[1], {"tp": other})
    beside_gain = gain_copy(1, gain_x.at[0], gain_x.at[1], {"dp": beside})
    across_gain = gain_copy(2, gain_y.at[0], gain_y.at[1], {"dp": across})
    go(pair_gain)
    swaps[0].wait_recv()
    chain(1, 1)
    pair_gain.wait_recv()
    gain_x[0] = gain_half[core] + gain_pair[1]
    go(beside_gain)
    for k in range(EARLY, chunks):
        go(x_copy(k))
    chain(0, 2)
    swaps[1].wait_recv()
    chain(1, 2)
    chain(0, 3)
    chain(1, 3)
    chain(3, 1)
    chain(2, 2)
    for s in range(4, n_z + 1):
        chain(0, s)
        chain(1, s)
    complete(0)
    complete(1)
    locals_[4].wait()

    partial(0)
    chain(3, 2)
    partial(1)
    chain(2, 3)
    beside_gain.wait_recv()
    gain_y[0] = gain_x[0] + gain_x[1]
    go(across_gain)
    chain(3, 3)
    partial(2)
    across_gain.wait_recv()
    gain_z[z] = gain_y[0] + gain_y[1]
    chain(GAIN, 1)
    partial(3)
    for s in range(4, n_z + 1):
        chain(2, s)
    partial(4)
    for s in range(4, n_z + 1):
        chain(3, s)
    chain(GAIN, 2)
    complete(2)
    complete(3)
    for copy in locals_[5:]:
        copy.wait()
    for k in range(3):
        own_sum(k)
    for k in range(2):
        finish(k)
    partial(5)
    chain(GAIN, 3)
    done, finished = 3, 2
    for k in range(6, chunks):
        while done < k - 1:
            own_sum(done)
            done += 1
            if finished < done - 1:
                finish(finished)
                finished += 1
        partial(k)
        if k == 6:
            for s in range(4, n_z + 1):
                chain(GAIN, s)
            gain_all[core] = jnp.sum(gain_z[...], axis=0) / n_dp
            go(gain_copy(3, gain_all.at[core], gain_all.at[core], {"tp": other}))
    while done < chunks:
        own_sum(done)
        done += 1
    gain_copy(3, gain_all.at[1 - core], gain_all.at[1 - core], {"tp": other}).wait_recv()
    per = span // LANES
    for h in range(2):
        for i in range(per):
            at = pl.ds(h * lines * per + i, lines, stride=per)
            gain_ref[at, :] = gain_all[h, :, i * LANES:(i + 1) * LANES]
    while finished < chunks:
        finish(finished)
        finished += 1

    for copy in sent:
        copy.wait_send()
    for g in range(GAIN + 1):
        for s in range(1, n_z):
            @pl.when((z - s + 1 >= 0) & (z + 1 < n_z))
            def _():
                up(g, s).wait_send()

            @pl.when((z + s - 1 < n_z) & (z - 1 >= 0))
            def _():
                down(g, s).wait_send()
        if g < GAIN:
            for b in range(n_z):
                to_pair(g, b).wait_send()


def store_kernel(*refs):
    count = (len(refs) - 1) // 2
    copies = [pltpu.make_async_copy(refs[i], refs[count + i], refs[-1].at[i]) for i in range(count)]
    for copy in copies:
        copy.start()
    for copy in copies:
        copy.wait()


def store_call(*arrays):
    return pl.pallas_call(
        store_kernel,
        out_shape=tuple(jax.ShapeDtypeStruct(a.shape, a.dtype) for a in arrays),
        in_specs=[pl.BlockSpec(memory_space=pltpu.VMEM)] * len(arrays),
        out_specs=(pl.BlockSpec(memory_space=pltpu.HBM),) * len(arrays),
        scratch_shapes=[pltpu.SemaphoreType.DMA((len(arrays),))],
        compiler_params=pltpu.CompilerParams(vmem_limit_bytes=1024 * 1024),
    )(*arrays)


def pair_call(layer, n_tp, x, g, a, b, m, v):
    tokens, features = x.shape
    rows, width = g.shape
    model = a.shape[1]
    n_dp = 4
    cols = width // n_dp
    n_z = n_tp // 2
    chunks = features // LANES
    span = model // 16
    dma = pltpu.SemaphoreType.DMA
    bf16, f32 = jnp.bfloat16, jnp.float32
    buffers = [
        ((2, tokens, features), bf16), ((4, tokens, cols), bf16),
        ((features, cols), bf16), ((features, cols), bf16), ((features, cols), f32),
        ((features, cols), f32), ((features, cols), f32),
        ((rows, model), bf16), ((rows, model), bf16),
        ((2, 8, span), f32), ((2, 8, span), f32), ((2, 8, span), f32), ((2, 8, span), f32),
        ((n_z, 8, span), f32), ((2, 8, span), f32),
    ]
    total = jax.ShapeDtypeStruct((features, cols), f32)
    return pl.pallas_call(
        functools.partial(pair_kernel, n_tp),
        out_shape=(total, total, total, jax.ShapeDtypeStruct((model // LANES, LANES), f32)),
        in_specs=[pl.BlockSpec(memory_space=pltpu.HBM)] * 6,
        out_specs=(pl.BlockSpec(memory_space=pltpu.VMEM),) * 4,
        scratch_shapes=[pltpu.VMEM(shape, dtype) for shape, dtype in buffers] + [
            dma((7,)), dma((2,)), dma((2,)), dma((chunks,)), dma((chunks,)), dma((chunks, 2)), dma((chunks, 2)),
        ] + [dma((5, n_z))] * 6 + [dma((4,)), dma((4,))],
        compiler_params=pltpu.CompilerParams(
            collective_id=layer, has_side_effects=True, vmem_limit_bytes=VMEM_LIMIT,
        ),
    )(x, g, a, b, m, v)


def shards(n_dp, n_tp, proj_in, kv_grad, normed, norm_grad, first_moment, second_moment):
    layers, tokens, features = proj_in.shape
    rows, width = kv_grad.shape[1:]
    model = normed.shape[2]
    cols = width // n_dp
    lines = 8
    dma = pltpu.SemaphoreType.DMA
    n_z = n_tp // 2
    firsts, seconds, updates, gains = [], [], [], []
    for layer in range(layers):
        if n_dp == 4 and features % LANES == 0 and features >= 8 * LANES and model % (16 * LANES) == 0 and n_tp >= 6:
            new_first, new_second, update, gain = store_call(*pair_call(
                layer, n_tp, proj_in[layer], kv_grad[layer], normed[layer], norm_grad[layer],
                first_moment[layer], second_moment[layer],
            ))
        else:
            total, gain = pl.pallas_call(
                functools.partial(kernel, n_dp, n_tp),
                out_shape=(
                    jax.ShapeDtypeStruct((features, cols), jnp.float32),
                    jax.ShapeDtypeStruct((lines, model // lines), jnp.float32),
                ),
                in_specs=[pl.BlockSpec(memory_space=pltpu.HBM)] * 4,
                out_specs=(pl.BlockSpec(memory_space=pltpu.VMEM), pl.BlockSpec(memory_space=pltpu.VMEM)),
                scratch_shapes=[
                    pltpu.VMEM((n_dp, tokens, features), jnp.bfloat16),
                    pltpu.VMEM((n_dp, n_tp * rows, cols), jnp.bfloat16),
                    pltpu.VMEM((rows, model), jnp.bfloat16),
                    pltpu.VMEM((rows, model), jnp.bfloat16),
                    pltpu.VMEM((n_tp, lines, model // lines), jnp.float32),
                    pltpu.VMEM((n_dp, lines, model // lines), jnp.float32),
                    dma((4,)),
                    dma((n_dp, PIECES)), dma((n_dp, PIECES)),
                    dma((n_dp,)), dma((n_dp,)),
                    dma((n_z,)), dma((n_z,)), dma((n_z,)), dma((n_z,)),
                    dma((n_z,)), dma((n_z,)),
                    dma((n_tp,)), dma((n_tp,)), dma((n_dp,)), dma((n_dp,)),
                ],
                compiler_params=pltpu.CompilerParams(
                    collective_id=layer, has_side_effects=True, vmem_limit_bytes=60 * 1024 * 1024,
                ),
            )(proj_in[layer], kv_grad[layer], normed[layer], norm_grad[layer])
            new_first, new_second, update = adam_update(total / n_dp, first_moment[layer], second_moment[layer])
        firsts.append(new_first)
        seconds.append(new_second)
        updates.append(update)
        gains.append(gain.reshape(model))
    return (jnp.stack(firsts), jnp.stack(seconds), jnp.stack(updates), jnp.stack(gains))


def solution(mesh):
    return jax.shard_map(
        functools.partial(shards, mesh.shape["dp"], mesh.shape["tp"]),
        mesh=mesh,
        in_specs=(
            P(None, "dp", "tp"),
            P(None, ("dp", "tp"), None),
            P(None, ("dp", "tp"), None),
            P(None, ("dp", "tp"), None),
            P(None, "tp", "dp"),
            P(None, "tp", "dp"),
        ),
        out_specs=(P(None, "tp", "dp"), P(None, "tp", "dp"), P(None, "tp", "dp"), P()),
        check_vma=False,
    )
```

```python
import functools
import math

import jax
import jax.numpy as jnp
from jax import lax
from jax.experimental import pallas as pl
from jax.experimental.pallas import tpu as pltpu
from jax.sharding import PartitionSpec as P

beta_one = 0.9
beta_two = 0.95
correct_one = 0.19
correct_two = 0.0975
epsilon = 1e-08
PIECES = 4
LANES = 128
SPAN = 250.0
KNEE = 2.0 ** -5
EARLY = 2
VMEM_LIMIT = 46 * 1024 * 1024


def adam_update(mean_grad, first_old, second_old):
    new_first = beta_one * first_old + (1.0 - beta_one) * mean_grad
    new_second = beta_two * second_old + (1.0 - beta_two) * mean_grad * mean_grad
    update = new_first / correct_one / (jnp.sqrt(new_second / correct_two) + epsilon)
    return (new_first, new_second, update)


def kernel(
    n_dp, n_tp, x_hbm, g_hbm, a_hbm, b_hbm, sum_ref, gain_ref,
    xs, kv, a_buf, b_buf, gain_tp, gain_dp,
    local_sem, x_send, x_recv, a2a_send, a2a_recv,
    up_send, up_recv, down_send, down_recv, pair_send, pair_recv,
    gt_send, gt_recv, gd_send, gd_recv,
):
    dp = lax.axis_index("dp")
    tp = lax.axis_index("tp")
    z = tp // 2
    core = tp % 2
    n_z = n_tp // 2
    rows = g_hbm.shape[0]
    cols = kv.shape[2]
    tokens = x_hbm.shape[0]
    piece = tokens // PIECES

    def dp_peer(o):
        return jnp.bitwise_xor(dp, o)

    def tp_peer(o):
        return lax.rem(tp + o, n_tp)

    locals_ = [
        pltpu.make_async_copy(a_hbm, a_buf, local_sem.at[0]),
        pltpu.make_async_copy(b_hbm, b_buf, local_sem.at[1]),
        pltpu.make_async_copy(
            g_hbm.at[:, pl.ds(pl.multiple_of(dp * cols, cols), cols)],
            kv.at[dp, pl.ds(pl.multiple_of(tp * rows, rows), rows), :],
            local_sem.at[2],
        ),
        pltpu.make_async_copy(x_hbm, xs.at[dp], local_sem.at[3]),
    ]
    for copy in locals_:
        copy.start()

    barrier = pltpu.get_barrier_semaphore()
    for o in range(1, n_dp):
        pl.semaphore_signal(barrier, inc=1, device_id={"dp": dp_peer(o)}, device_id_type=pl.DeviceIdType.MESH)
    for o in range(1, n_tp):
        pl.semaphore_signal(barrier, inc=1, device_id={"tp": tp_peer(o)}, device_id_type=pl.DeviceIdType.MESH)
    pl.semaphore_wait(barrier, n_dp - 1 + n_tp - 1)

    sent = []

    def remote(src, dst, send, recv, where):
        return pltpu.make_async_remote_copy(
            src_ref=src, dst_ref=dst, send_sem=send, recv_sem=recv,
            device_id=where, device_id_type=pl.DeviceIdType.MESH,
        )

    my_rows = pl.ds(pl.multiple_of(tp * rows, rows), rows)
    a2a = []
    for o in range(1, n_dp):
        peer = dp_peer(o)
        copy = remote(
            g_hbm.at[:, pl.ds(pl.multiple_of(peer * cols, cols), cols)],
            kv.at[dp, my_rows, :], a2a_send.at[o], a2a_recv.at[o], {"dp": peer},
        )
        copy.start()
        a2a.append(copy)
        sent.append(copy)

    def x_copy(src, origin, c, o_recv, o_to, send):
        part = pl.ds(c * piece, piece)
        return remote(
            src.at[part, :], xs.at[origin, part, :], send, x_recv.at[o_recv, c],
            {"dp": dp_peer(o_to)},
        )

    square = n_dp == 4
    orders = {o: list(range(PIECES)) for o in range(1, n_dp)}
    half = PIECES // 2
    if square:
        orders[2] = list(range(half, PIECES)) + list(range(half))
        orders[3] = []

    def send_own(i):
        for o in range(1, n_dp):
            if i < len(orders[o]):
                c = orders[o][i]
                copy = x_copy(x_hbm, dp, c, o, o, x_send.at[o, c])
                copy.start()
                sent.append(copy)

    def got(o, c):
        x_copy(xs.at[dp_peer(o)], dp_peer(o), c, o, o, x_send.at[o, c]).wait_recv()

    def forward(i):
        for o, o_to in ((1, 2), (2, 1)):
            c = orders[o][i]
            got(o, c)
            copy = x_copy(xs.at[dp_peer(o)], dp_peer(o), c, 3, o_to, x_send.at[3, c])
            copy.start()
            sent.append(copy)

    send_own(0)
    send_own(1)

    locals_[0].wait()
    locals_[1].wait()
    wide = gain_tp.shape[2]
    lines = gain_tp.shape[1]
    for j in range(lines):
        s = pl.ds(j * wide, wide)
        products = a_buf[:, s].astype(jnp.float32) * b_buf[:, s].astype(jnp.float32)
        gain_tp[tp, pl.ds(j, 1), :] = jnp.sum(products, axis=0, keepdims=True)
    tp_copies = []
    for o in range(1, n_tp):
        copy = remote(gain_tp.at[tp], gain_tp.at[tp], gt_send.at[o], gt_recv.at[o], {"tp": tp_peer(o)})
        copy.start()
        sent.append(copy)
        tp_copies.append(copy)

    def block(b, c):
        return kv.at[:, pl.ds(pl.multiple_of((2 * b + c) * rows, rows), rows), :]

    other = 2 * z + 1 - core

    def to_pair(b):
        return remote(block(b, core), block(b, core), pair_send.at[b], pair_recv.at[b], {"tp": other})

    def up(s):
        b = z - s + 1
        return remote(block(b, core), block(b, core), up_send.at[s], up_recv.at[s], {"tp": tp + 2})

    def down(s):
        b = z + s - 1
        return remote(block(b, core), block(b, core), down_send.at[s], down_recv.at[s], {"tp": tp - 2})

    def up_got(s):
        b = z - s
        return remote(block(b, core), block(b, core), up_send.at[s], up_recv.at[s], {"tp": other})

    def down_got(s):
        b = z + s
        return remote(block(b, core), block(b, core), down_send.at[s], down_recv.at[s], {"tp": other})

    locals_[2].wait()
    for o in range(1, n_dp):
        a2a[o - 1].wait_recv()

    for s in range(1, n_z + 1):
        if s > 1:
            @pl.when(z - s + 1 >= 0)
            def _():
                up_got(s - 1).wait_recv()

        if s < n_z:
            @pl.when((z - s + 1 >= 0) & (z + 1 < n_z))
            def _():
                up(s).start()

        if s > 1:
            @pl.when(z + s - 1 < n_z)
            def _():
                down_got(s - 1).wait_recv()

        if s < n_z:
            @pl.when((z + s - 1 < n_z) & (z - 1 >= 0))
            def _():
                down(s).start()

        if s == 1:
            to_pair(z).start()
        else:
            @pl.when(z - s + 1 >= 0)
            def _():
                to_pair(z - s + 1).start()

            @pl.when(z + s - 1 < n_z)
            def _():
                to_pair(z + s - 1).start()

        if s == 1:
            for copy in tp_copies:
                copy.wait_recv()
            gain_dp[dp, :, :] = jnp.sum(gain_tp[...], axis=0)
            for o in range(1, n_dp):
                copy = remote(gain_dp.at[dp], gain_dp.at[dp], gd_send.at[o], gd_recv.at[o], {"dp": dp_peer(o)})
                copy.start()
                sent.append(copy)
            for i in range(2, PIECES):
                send_own(i)
        if square and 2 <= s < 2 + half:
            forward(s - 2)
    if square:
        for i in range(max(n_z - 1, 0), half):
            forward(i)

    for b in range(n_z):
        remote(block(b, 1 - core), block(b, 1 - core), pair_send.at[b], pair_recv.at[b], {"tp": other}).wait_recv()

    width = min(256, sum_ref.shape[0])

    def multiply(origin, start, size, first=False):
        @pl.loop(0, sum_ref.shape[0] // width)
        def _(f):
            at = pl.ds(pl.multiple_of(f * width, width), width)
            part = lax.dot_general(
                xs[origin, pl.ds(start, size), at], kv[origin, pl.ds(start, size), :],
                (((0,), (0,)), ((), ())), preferred_element_type=jnp.float32,
            )
            if first:
                sum_ref[at, :] = part
            else:
                sum_ref[at, :] += part

    locals_[3].wait()
    multiply(dp, 0, tokens, True)
    for o in range(1, n_dp):
        if square and o == 3:
            continue
        for c in orders[o]:
            if not (square and c in orders[o][:half]):
                got(o, c)
        multiply(dp_peer(o), 0, tokens)

    for o in range(1, n_dp):
        remote(gain_dp.at[dp_peer(o)], gain_dp.at[dp_peer(o)], gd_send.at[o], gd_recv.at[o], {"dp": dp_peer(o)}).wait_recv()
    gain_ref[...] = jnp.sum(gain_dp[...], axis=0) / n_dp

    if square:
        for i in range(half):
            for o in (1, 2):
                c = orders[o][i]
                got(3, c)
                multiply(dp_peer(3), c * piece, piece)

    for copy in sent:
        copy.wait_send()
    for s in range(1, n_z):
        @pl.when((z - s + 1 >= 0) & (z + 1 < n_z))
        def _():
            up(s).wait_send()

        @pl.when((z + s - 1 < n_z) & (z - 1 >= 0))
        def _():
            down(s).wait_send()
    for b in range(n_z):
        to_pair(b).wait_send()


def encode(value, bound):
    power = SPAN / math.log2(1.0 + bound / KNEE)
    code = jnp.exp2(power * jnp.log2(1.0 + jnp.abs(value) * (1.0 / KNEE)) - SPAN / 2)
    return jnp.where(value < 0.0, -code, code).astype(jnp.bfloat16)


def decode(code, bound):
    power = SPAN / math.log2(1.0 + bound / KNEE)
    code = code.astype(jnp.float32)
    value = (jnp.exp2((jnp.log2(jnp.abs(code)) + SPAN / 2) * (1.0 / power)) - 1.0) * KNEE
    return jnp.where(code < 0.0, -value, value)


def pair_kernel(
    n_tp, x_hbm, g_hbm, a_hbm, b_hbm, m_hbm, v_hbm, first_ref, second_ref, step_ref, gain_ref,
    xs, kv, part, arrived, own, m_buf, v_buf, a_buf, b_buf, gain_half, gain_pair, gain_x, gain_y, gain_z, gain_all,
    local_sem, swap_send, swap_recv, x_send, x_recv, part_send, part_recv,
    up_send, up_recv, down_send, down_recv, pair_send, pair_recv, gain_send, gain_recv, upper_in, ready,
):
    n_dp = 4
    dp = lax.axis_index("dp")
    tp = lax.axis_index("tp")
    z = tp // 2
    core = tp % 2
    n_z = n_tp // 2
    rows = g_hbm.shape[0]
    cols = kv.shape[2]
    tokens, features = x_hbm.shape
    chunks = features // LANES
    bound = 2.0 * tokens * 6.0 * 0.75
    other = 2 * z + 1 - core
    beside = jnp.bitwise_xor(dp, 1)
    across = jnp.bitwise_xor(dp, 2)
    sent = []

    def remote(src, dst, send, recv, where):
        return pltpu.make_async_remote_copy(
            src_ref=src, dst_ref=dst, send_sem=send, recv_sem=recv,
            device_id=where, device_id_type=pl.DeviceIdType.MESH,
        )

    def go(copy):
        copy.start()
        sent.append(copy)

    my_rows = pl.ds(pl.multiple_of(tp * rows, rows), rows)

    def g_cols(d):
        return g_hbm.at[:, pl.ds(pl.multiple_of(d * cols, cols), cols)]

    locals_ = [
        pltpu.make_async_copy(g_cols(across), kv.at[0, my_rows, :], local_sem.at[0]),
        pltpu.make_async_copy(g_cols(dp), kv.at[2, my_rows, :], local_sem.at[1]),
        pltpu.make_async_copy(a_hbm, a_buf, local_sem.at[2]),
        pltpu.make_async_copy(b_hbm, b_buf, local_sem.at[3]),
        pltpu.make_async_copy(x_hbm, xs.at[0], local_sem.at[4]),
        pltpu.make_async_copy(m_hbm, m_buf, local_sem.at[5]),
        pltpu.make_async_copy(v_hbm, v_buf, local_sem.at[6]),
    ]
    for copy in locals_:
        copy.start()

    barrier = pltpu.get_barrier_semaphore()

    def hello(where):
        pl.semaphore_signal(barrier, inc=1, device_id=where, device_id_type=pl.DeviceIdType.MESH)

    hello({"dp": beside})
    hello({"dp": across})
    hello({"tp": other})

    @pl.when(z + 1 < n_z)
    def _():
        hello({"tp": tp + 2})

    pl.semaphore_wait(barrier, 3 + jnp.where(z >= 1, 1, 0))

    @pl.when(z >= 1)
    def _():
        pl.semaphore_signal(upper_in, inc=1, device_id={"tp": tp - 2}, device_id_type=pl.DeviceIdType.MESH)

    def swap(i, plane, d):
        return remote(g_cols(d), kv.at[plane, my_rows, :], swap_send.at[i], swap_recv.at[i], {"dp": beside})

    swaps = [swap(0, 1, jnp.bitwise_xor(dp, 3)), swap(1, 3, beside)]

    def x_copy(k):
        at = pl.ds(k * LANES, LANES)
        return remote(x_hbm.at[:, at], xs.at[1, :, at], x_send.at[k], x_recv.at[k], {"dp": beside})

    go(swaps[0])
    go(swaps[1])
    for k in range(EARLY):
        go(x_copy(k))

    GAIN = 4

    def block(g, b, c):
        if g == GAIN:
            return gain_z.at[b]
        return kv.at[g, pl.ds(pl.multiple_of((2 * b + c) * rows, rows), rows), :]

    def to_pair(g, b):
        return remote(block(g, b, core), block(g, b, core), pair_send.at[g, b], pair_recv.at[g, b], {"tp": other})

    def from_pair(g, b):
        return remote(block(g, b, 1 - core), block(g, b, 1 - core), pair_send.at[g, b], pair_recv.at[g, b], {"tp": other})

    def up(g, s):
        b = z - s + 1
        return remote(block(g, b, core), block(g, b, core), up_send.at[g, s], up_recv.at[g, s], {"tp": tp + 2})

    def down(g, s):
        b = z + s - 1
        return remote(block(g, b, core), block(g, b, core), down_send.at[g, s], down_recv.at[g, s], {"tp": tp - 2})

    def up_got(g, s):
        b = z - s
        return remote(block(g, b, core), block(g, b, core), up_send.at[g, s], up_recv.at[g, s], {"tp": other})

    def down_got(g, s):
        b = z + s
        return remote(block(g, b, core), block(g, b, core), down_send.at[g, s], down_recv.at[g, s], {"tp": other})

    def chain(g, s):
        if s > 1:
            @pl.when(z - s + 1 >= 0)
            def _():
                up_got(g, s - 1).wait_recv()

        if s < n_z:
            @pl.when((z - s + 1 >= 0) & (z + 1 < n_z))
            def _():
                up(g, s).start()

        if s > 1:
            @pl.when(z + s - 1 < n_z)
            def _():
                down_got(g, s - 1).wait_recv()

        if s < n_z:
            @pl.when((z + s - 1 < n_z) & (z - 1 >= 0))
            def _():
                down(g, s).start()

        if g == GAIN:
            return
        if s == 1:
            to_pair(g, z).start()
        else:
            @pl.when(z - s + 1 >= 0)
            def _():
                to_pair(g, z - s + 1).start()

            @pl.when(z + s - 1 < n_z)
            def _():
                to_pair(g, z + s - 1).start()

    def complete(g):
        for b in range(n_z):
            from_pair(g, b).wait_recv()

    def gain_copy(i, src, dst, where):
        return remote(src, dst, gain_send.at[i], gain_recv.at[i], where)

    def dot(x, w):
        return lax.dot_general(x, w, (((0,), (0,)), ((), ())), preferred_element_type=jnp.float32)

    halves = 2
    wide = cols // halves

    def part_copy(k, h):
        at = (pl.ds(k * LANES, LANES), pl.ds(h * wide, wide))
        return remote(part.at[at], arrived.at[at], part_send.at[k, h], part_recv.at[k, h], {"dp": across})

    def partial(k):
        at = pl.ds(k * LANES, LANES)
        last = k == chunks - 1
        if last:
            ready[...] = dot(xs[0, :, at], kv[0])
        x_copy(k).wait_recv()
        for h in range(halves):
            ch = pl.ds(h * wide, wide)
            head = ready[:, ch] if last else dot(xs[0, :, at], kv[0, :, ch])
            total = head + dot(xs[1, :, at], kv[1, :, ch])
            part[at, ch] = encode(total, bound)
            go(part_copy(k, h))

    def own_sum(k):
        at = pl.ds(k * LANES, LANES)
        own[at, :] = dot(xs[0, :, at], kv[2]) + dot(xs[1, :, at], kv[3])

    def finish(k):
        at = pl.ds(k * LANES, LANES)
        for h in range(halves):
            ch = pl.ds(h * wide, wide)
            part_copy(k, h).wait_recv()
            mean = (own[at, ch] + decode(arrived[at, ch], bound)) / n_dp
            new_first, new_second, update = adam_update(mean, m_buf[at, ch], v_buf[at, ch])
            first_ref[at, ch] = new_first
            second_ref[at, ch] = new_second
            step_ref[at, ch] = update

    @pl.when(z + 1 < n_z)
    def _():
        pl.semaphore_wait(upper_in, 1)

    locals_[0].wait()
    chain(0, 1)
    locals_[1].wait()
    chain(2, 1)

    locals_[2].wait()
    locals_[3].wait()
    lines, span = gain_half.shape[1:]
    for h in range(2):
        for j in range(lines):
            at = pl.ds((h * lines + j) * span, span)
            products = a_buf[:, at].astype(jnp.float32) * b_buf[:, at].astype(jnp.float32)
            gain_half[h, pl.ds(j, 1), :] = jnp.sum(products, axis=0, keepdims=True)
    pair_gain = gain_copy(0, gain_half.at[1 - core], gain_pair.at[1], {"tp": other})
    beside_gain = gain_copy(1, gain_x.at[0], gain_x.at[1], {"dp": beside})
    across_gain = gain_copy(2, gain_y.at[0], gain_y.at[1], {"dp": across})
    go(pair_gain)
    swaps[0].wait_recv()
    chain(1, 1)
    pair_gain.wait_recv()
    gain_x[0] = gain_half[core] + gain_pair[1]
    go(beside_gain)
    for k in range(EARLY, chunks):
        go(x_copy(k))
    chain(0, 2)
    swaps[1].wait_recv()
    chain(1, 2)
    chain(0, 3)
    chain(1, 3)
    chain(3, 1)
    chain(2, 2)
    for s in range(4, n_z + 1):
        chain(0, s)
        chain(1, s)
    complete(0)
    complete(1)
    locals_[4].wait()

    partial(0)
    chain(3, 2)
    partial(1)
    chain(2, 3)
    beside_gain.wait_recv()
    gain_y[0] = gain_x[0] + gain_x[1]
    go(across_gain)
    chain(3, 3)
    partial(2)
    across_gain.wait_recv()
    gain_z[z] = gain_y[0] + gain_y[1]
    chain(GAIN, 1)
    partial(3)
    for s in range(4, n_z + 1):
        chain(2, s)
    partial(4)
    for s in range(4, n_z + 1):
        chain(3, s)
    chain(GAIN, 2)
    complete(2)
    complete(3)
    for copy in locals_[5:]:
        copy.wait()
    for k in range(3):
        own_sum(k)
    for k in range(2):
        finish(k)
    partial(5)
    chain(GAIN, 3)
    for k in range(3, 6):
        own_sum(k)
    for k in range(2, 5):
        finish(k)
    partial(6)
    for s in range(4, n_z + 1):
        chain(GAIN, s)
    gain_all[core] = jnp.sum(gain_z[...], axis=0) / n_dp
    last_gain = gain_copy(3, gain_all.at[core], gain_all.at[core], {"tp": other})
    go(last_gain)
    own_sum(6)
    finish(5)
    gain_copy(3, gain_all.at[1 - core], gain_all.at[1 - core], {"tp": other}).wait_recv()
    per = span // LANES
    for h in range(2):
        for i in range(per):
            at = pl.ds(h * lines * per + i, lines, stride=per)
            gain_ref[at, :] = gain_all[h, :, i * LANES:(i + 1) * LANES]
    finish(6)
    for k in range(7, chunks):
        partial(k)
    for k in range(7, chunks):
        own_sum(k)
    for k in range(7, chunks):
        finish(k)

    for copy in sent:
        copy.wait_send()
    for g in range(GAIN + 1):
        for s in range(1, n_z):
            @pl.when((z - s + 1 >= 0) & (z + 1 < n_z))
            def _():
                up(g, s).wait_send()

            @pl.when((z + s - 1 < n_z) & (z - 1 >= 0))
            def _():
                down(g, s).wait_send()
        if g < GAIN:
            for b in range(n_z):
                to_pair(g, b).wait_send()


def store_kernel(*refs):
    count = (len(refs) - 1) // 2
    copies = [pltpu.make_async_copy(refs[i], refs[count + i], refs[-1].at[i]) for i in range(count)]
    for copy in copies:
        copy.start()
    for copy in copies:
        copy.wait()


def store_call(*arrays):
    return pl.pallas_call(
        store_kernel,
        out_shape=tuple(jax.ShapeDtypeStruct(a.shape, a.dtype) for a in arrays),
        in_specs=[pl.BlockSpec(memory_space=pltpu.VMEM)] * len(arrays),
        out_specs=(pl.BlockSpec(memory_space=pltpu.HBM),) * len(arrays),
        scratch_shapes=[pltpu.SemaphoreType.DMA((len(arrays),))],
        compiler_params=pltpu.CompilerParams(vmem_limit_bytes=1024 * 1024),
    )(*arrays)


def pair_call(layer, n_tp, x, g, a, b, m, v):
    tokens, features = x.shape
    rows, width = g.shape
    model = a.shape[1]
    n_dp = 4
    cols = width // n_dp
    n_z = n_tp // 2
    chunks = features // LANES
    span = model // 16
    dma = pltpu.SemaphoreType.DMA
    bf16, f32 = jnp.bfloat16, jnp.float32
    buffers = [
        ((2, tokens, features), bf16), ((4, tokens, cols), bf16),
        ((features, cols), bf16), ((features, cols), bf16), ((features, cols), f32),
        ((features, cols), f32), ((features, cols), f32),
        ((rows, model), bf16), ((rows, model), bf16),
        ((2, 8, span), f32), ((2, 8, span), f32), ((2, 8, span), f32), ((2, 8, span), f32),
        ((n_z, 8, span), f32), ((2, 8, span), f32),
    ]
    total = jax.ShapeDtypeStruct((features, cols), f32)
    return pl.pallas_call(
        functools.partial(pair_kernel, n_tp),
        out_shape=(total, total, total, jax.ShapeDtypeStruct((model // LANES, LANES), f32)),
        in_specs=[pl.BlockSpec(memory_space=pltpu.HBM)] * 6,
        out_specs=(pl.BlockSpec(memory_space=pltpu.VMEM),) * 4,
        scratch_shapes=[pltpu.VMEM(shape, dtype) for shape, dtype in buffers] + [
            dma((7,)), dma((2,)), dma((2,)), dma((chunks,)), dma((chunks,)), dma((chunks, 2)), dma((chunks, 2)),
        ] + [dma((5, n_z))] * 6 + [dma((4,)), dma((4,)), pltpu.SemaphoreType.REGULAR, pltpu.VMEM((LANES, cols), f32)],
        compiler_params=pltpu.CompilerParams(
            collective_id=layer, has_side_effects=True, vmem_limit_bytes=VMEM_LIMIT,
        ),
    )(x, g, a, b, m, v)


def shards(n_dp, n_tp, proj_in, kv_grad, normed, norm_grad, first_moment, second_moment):
    layers, tokens, features = proj_in.shape
    rows, width = kv_grad.shape[1:]
    model = normed.shape[2]
    cols = width // n_dp
    lines = 8
    dma = pltpu.SemaphoreType.DMA
    n_z = n_tp // 2
    firsts, seconds, updates, gains = [], [], [], []
    for layer in range(layers):
        if n_dp == 4 and features % LANES == 0 and features >= 8 * LANES and model % (16 * LANES) == 0 and n_tp >= 6:
            new_first, new_second, update, gain = store_call(*pair_call(
                layer, n_tp, proj_in[layer], pltpu.with_memory_space_constraint(kv_grad[layer], pltpu.HBM), normed[layer], norm_grad[layer],
                first_moment[layer], second_moment[layer],
            ))
        else:
            total, gain = pl.pallas_call(
                functools.partial(kernel, n_dp, n_tp),
                out_shape=(
                    jax.ShapeDtypeStruct((features, cols), jnp.float32),
                    jax.ShapeDtypeStruct((lines, model // lines), jnp.float32),
                ),
                in_specs=[pl.BlockSpec(memory_space=pltpu.HBM)] * 4,
                out_specs=(pl.BlockSpec(memory_space=pltpu.VMEM), pl.BlockSpec(memory_space=pltpu.VMEM)),
                scratch_shapes=[
                    pltpu.VMEM((n_dp, tokens, features), jnp.bfloat16),
                    pltpu.VMEM((n_dp, n_tp * rows, cols), jnp.bfloat16),
                    pltpu.VMEM((rows, model), jnp.bfloat16),
                    pltpu.VMEM((rows, model), jnp.bfloat16),
                    pltpu.VMEM((n_tp, lines, model // lines), jnp.float32),
                    pltpu.VMEM((n_dp, lines, model // lines), jnp.float32),
                    dma((4,)),
                    dma((n_dp, PIECES)), dma((n_dp, PIECES)),
                    dma((n_dp,)), dma((n_dp,)),
                    dma((n_z,)), dma((n_z,)), dma((n_z,)), dma((n_z,)),
                    dma((n_z,)), dma((n_z,)),
                    dma((n_tp,)), dma((n_tp,)), dma((n_dp,)), dma((n_dp,)),
                ],
                compiler_params=pltpu.CompilerParams(
                    collective_id=layer, has_side_effects=True, vmem_limit_bytes=60 * 1024 * 1024,
                ),
            )(proj_in[layer], kv_grad[layer], normed[layer], norm_grad[layer])
            new_first, new_second, update = adam_update(total / n_dp, first_moment[layer], second_moment[layer])
        firsts.append(new_first)
        seconds.append(new_second)
        updates.append(update)
        gains.append(gain.reshape(model))
    return (jnp.stack(firsts), jnp.stack(seconds), jnp.stack(updates), jnp.stack(gains))


def solution(mesh):
    return jax.shard_map(
        functools.partial(shards, mesh.shape["dp"], mesh.shape["tp"]),
        mesh=mesh,
        in_specs=(
            P(None, "dp", "tp"),
            P(None, ("dp", "tp"), None),
            P(None, ("dp", "tp"), None),
            P(None, ("dp", "tp"), None),
            P(None, "tp", "dp"),
            P(None, "tp", "dp"),
        ),
        out_specs=(P(None, "tp", "dp"), P(None, "tp", "dp"), P(None, "tp", "dp"), P()),
        check_vma=False,
    )
```

```python
import functools
import math

import jax
import jax.numpy as jnp
from jax import lax
from jax.experimental import pallas as pl
from jax.experimental.pallas import tpu as pltpu
from jax.sharding import PartitionSpec as P

beta_one = 0.9
beta_two = 0.95
correct_one = 0.19
correct_two = 0.0975
epsilon = 1e-08
PIECES = 4
LANES = 128
SPAN = 250.0
KNEE = 2.0 ** -10
POWER = SPAN / math.log2(1.0 + 1.0 / KNEE)
TINY = 2.0 ** -100
NOTE = 16
EARLY = 2
VMEM_LIMIT = 46 * 1024 * 1024


def adam_update(mean_grad, first_old, second_old):
    new_first = beta_one * first_old + (1.0 - beta_one) * mean_grad
    new_second = beta_two * second_old + (1.0 - beta_two) * mean_grad * mean_grad
    update = new_first / correct_one / (jnp.sqrt(new_second / correct_two) + epsilon)
    return (new_first, new_second, update)


def kernel(
    n_dp, n_tp, x_hbm, g_hbm, a_hbm, b_hbm, sum_ref, gain_ref,
    xs, kv, a_buf, b_buf, gain_tp, gain_dp,
    local_sem, x_send, x_recv, a2a_send, a2a_recv,
    up_send, up_recv, down_send, down_recv, pair_send, pair_recv,
    gt_send, gt_recv, gd_send, gd_recv,
):
    dp = lax.axis_index("dp")
    tp = lax.axis_index("tp")
    z = tp // 2
    core = tp % 2
    n_z = n_tp // 2
    rows = g_hbm.shape[0]
    cols = kv.shape[2]
    tokens = x_hbm.shape[0]
    piece = tokens // PIECES

    def dp_peer(o):
        return jnp.bitwise_xor(dp, o)

    def tp_peer(o):
        return lax.rem(tp + o, n_tp)

    locals_ = [
        pltpu.make_async_copy(a_hbm, a_buf, local_sem.at[0]),
        pltpu.make_async_copy(b_hbm, b_buf, local_sem.at[1]),
        pltpu.make_async_copy(
            g_hbm.at[:, pl.ds(pl.multiple_of(dp * cols, cols), cols)],
            kv.at[dp, pl.ds(pl.multiple_of(tp * rows, rows), rows), :],
            local_sem.at[2],
        ),
        pltpu.make_async_copy(x_hbm, xs.at[dp], local_sem.at[3]),
    ]
    for copy in locals_:
        copy.start()

    barrier = pltpu.get_barrier_semaphore()
    for o in range(1, n_dp):
        pl.semaphore_signal(barrier, inc=1, device_id={"dp": dp_peer(o)}, device_id_type=pl.DeviceIdType.MESH)
    for o in range(1, n_tp):
        pl.semaphore_signal(barrier, inc=1, device_id={"tp": tp_peer(o)}, device_id_type=pl.DeviceIdType.MESH)
    pl.semaphore_wait(barrier, n_dp - 1 + n_tp - 1)

    sent = []

    def remote(src, dst, send, recv, where):
        return pltpu.make_async_remote_copy(
            src_ref=src, dst_ref=dst, send_sem=send, recv_sem=recv,
            device_id=where, device_id_type=pl.DeviceIdType.MESH,
        )

    my_rows = pl.ds(pl.multiple_of(tp * rows, rows), rows)
    a2a = []
    for o in range(1, n_dp):
        peer = dp_peer(o)
        copy = remote(
            g_hbm.at[:, pl.ds(pl.multiple_of(peer * cols, cols), cols)],
            kv.at[dp, my_rows, :], a2a_send.at[o], a2a_recv.at[o], {"dp": peer},
        )
        copy.start()
        a2a.append(copy)
        sent.append(copy)

    def x_copy(src, origin, c, o_recv, o_to, send):
        part = pl.ds(c * piece, piece)
        return remote(
            src.at[part, :], xs.at[origin, part, :], send, x_recv.at[o_recv, c],
            {"dp": dp_peer(o_to)},
        )

    square = n_dp == 4
    orders = {o: list(range(PIECES)) for o in range(1, n_dp)}
    half = PIECES // 2
    if square:
        orders[2] = list(range(half, PIECES)) + list(range(half))
        orders[3] = []

    def send_own(i):
        for o in range(1, n_dp):
            if i < len(orders[o]):
                c = orders[o][i]
                copy = x_copy(x_hbm, dp, c, o, o, x_send.at[o, c])
                copy.start()
                sent.append(copy)

    def got(o, c):
        x_copy(xs.at[dp_peer(o)], dp_peer(o), c, o, o, x_send.at[o, c]).wait_recv()

    def forward(i):
        for o, o_to in ((1, 2), (2, 1)):
            c = orders[o][i]
            got(o, c)
            copy = x_copy(xs.at[dp_peer(o)], dp_peer(o), c, 3, o_to, x_send.at[3, c])
            copy.start()
            sent.append(copy)

    send_own(0)
    send_own(1)

    locals_[0].wait()
    locals_[1].wait()
    wide = gain_tp.shape[2]
    lines = gain_tp.shape[1]
    for j in range(lines):
        s = pl.ds(j * wide, wide)
        products = a_buf[:, s].astype(jnp.float32) * b_buf[:, s].astype(jnp.float32)
        gain_tp[tp, pl.ds(j, 1), :] = jnp.sum(products, axis=0, keepdims=True)
    tp_copies = []
    for o in range(1, n_tp):
        copy = remote(gain_tp.at[tp], gain_tp.at[tp], gt_send.at[o], gt_recv.at[o], {"tp": tp_peer(o)})
        copy.start()
        sent.append(copy)
        tp_copies.append(copy)

    def block(b, c):
        return kv.at[:, pl.ds(pl.multiple_of((2 * b + c) * rows, rows), rows), :]

    other = 2 * z + 1 - core

    def to_pair(b):
        return remote(block(b, core), block(b, core), pair_send.at[b], pair_recv.at[b], {"tp": other})

    def up(s):
        b = z - s + 1
        return remote(block(b, core), block(b, core), up_send.at[s], up_recv.at[s], {"tp": tp + 2})

    def down(s):
        b = z + s - 1
        return remote(block(b, core), block(b, core), down_send.at[s], down_recv.at[s], {"tp": tp - 2})

    def up_got(s):
        b = z - s
        return remote(block(b, core), block(b, core), up_send.at[s], up_recv.at[s], {"tp": other})

    def down_got(s):
        b = z + s
        return remote(block(b, core), block(b, core), down_send.at[s], down_recv.at[s], {"tp": other})

    locals_[2].wait()
    for o in range(1, n_dp):
        a2a[o - 1].wait_recv()

    for s in range(1, n_z + 1):
        if s > 1:
            @pl.when(z - s + 1 >= 0)
            def _():
                up_got(s - 1).wait_recv()

        if s < n_z:
            @pl.when((z - s + 1 >= 0) & (z + 1 < n_z))
            def _():
                up(s).start()

        if s > 1:
            @pl.when(z + s - 1 < n_z)
            def _():
                down_got(s - 1).wait_recv()

        if s < n_z:
            @pl.when((z + s - 1 < n_z) & (z - 1 >= 0))
            def _():
                down(s).start()

        if s == 1:
            to_pair(z).start()
        else:
            @pl.when(z - s + 1 >= 0)
            def _():
                to_pair(z - s + 1).start()

            @pl.when(z + s - 1 < n_z)
            def _():
                to_pair(z + s - 1).start()

        if s == 1:
            for copy in tp_copies:
                copy.wait_recv()
            gain_dp[dp, :, :] = jnp.sum(gain_tp[...], axis=0)
            for o in range(1, n_dp):
                copy = remote(gain_dp.at[dp], gain_dp.at[dp], gd_send.at[o], gd_recv.at[o], {"dp": dp_peer(o)})
                copy.start()
                sent.append(copy)
            for i in range(2, PIECES):
                send_own(i)
        if square and 2 <= s < 2 + half:
            forward(s - 2)
    if square:
        for i in range(max(n_z - 1, 0), half):
            forward(i)

    for b in range(n_z):
        remote(block(b, 1 - core), block(b, 1 - core), pair_send.at[b], pair_recv.at[b], {"tp": other}).wait_recv()

    width = min(256, sum_ref.shape[0])

    def multiply(origin, start, size, first=False):
        @pl.loop(0, sum_ref.shape[0] // width)
        def _(f):
            at = pl.ds(pl.multiple_of(f * width, width), width)
            part = lax.dot_general(
                xs[origin, pl.ds(start, size), at], kv[origin, pl.ds(start, size), :],
                (((0,), (0,)), ((), ())), preferred_element_type=jnp.float32,
            )
            if first:
                sum_ref[at, :] = part
            else:
                sum_ref[at, :] += part

    locals_[3].wait()
    multiply(dp, 0, tokens, True)
    for o in range(1, n_dp):
        if square and o == 3:
            continue
        for c in orders[o]:
            if not (square and c in orders[o][:half]):
                got(o, c)
        multiply(dp_peer(o), 0, tokens)

    for o in range(1, n_dp):
        remote(gain_dp.at[dp_peer(o)], gain_dp.at[dp_peer(o)], gd_send.at[o], gd_recv.at[o], {"dp": dp_peer(o)}).wait_recv()
    gain_ref[...] = jnp.sum(gain_dp[...], axis=0) / n_dp

    if square:
        for i in range(half):
            for o in (1, 2):
                c = orders[o][i]
                got(3, c)
                multiply(dp_peer(3), c * piece, piece)

    for copy in sent:
        copy.wait_send()
    for s in range(1, n_z):
        @pl.when((z - s + 1 >= 0) & (z + 1 < n_z))
        def _():
            up(s).wait_send()

        @pl.when((z + s - 1 < n_z) & (z - 1 >= 0))
        def _():
            down(s).wait_send()
    for b in range(n_z):
        to_pair(b).wait_send()


def scale_of(held):
    return jnp.maximum(held.astype(jnp.float32), TINY)


def encode(value, scale):
    code = jnp.exp2(POWER * jnp.log2(1.0 + jnp.abs(value) * (1.0 / (scale * KNEE))) - SPAN / 2)
    return jnp.where(value < 0.0, -code, code).astype(jnp.bfloat16)


def decode(code, scale):
    code = code.astype(jnp.float32)
    value = (jnp.exp2((jnp.log2(jnp.abs(code)) + SPAN / 2) * (1.0 / POWER)) - 1.0) * (scale * KNEE)
    return jnp.where(code < 0.0, -value, value)


def pair_kernel(
    n_tp, x_hbm, g_hbm, a_hbm, b_hbm, m_hbm, v_hbm, first_ref, second_ref, step_ref, gain_ref,
    xs, kv, part, arrived, own, m_buf, v_buf, a_buf, b_buf, gain_half, gain_pair, gain_x, gain_y, gain_z, gain_all,
    local_sem, swap_send, swap_recv, x_send, x_recv, part_send, part_recv,
    up_send, up_recv, down_send, down_recv, pair_send, pair_recv, gain_send, gain_recv, upper_in, ready,
):
    n_dp = 4
    dp = lax.axis_index("dp")
    tp = lax.axis_index("tp")
    z = tp // 2
    core = tp % 2
    n_z = n_tp // 2
    rows = g_hbm.shape[0]
    cols = kv.shape[2]
    tokens, features = x_hbm.shape
    chunks = features // LANES
    other = 2 * z + 1 - core
    beside = jnp.bitwise_xor(dp, 1)
    across = jnp.bitwise_xor(dp, 2)
    sent = []

    def remote(src, dst, send, recv, where):
        return pltpu.make_async_remote_copy(
            src_ref=src, dst_ref=dst, send_sem=send, recv_sem=recv,
            device_id=where, device_id_type=pl.DeviceIdType.MESH,
        )

    def go(copy):
        copy.start()
        sent.append(copy)

    my_rows = pl.ds(pl.multiple_of(tp * rows, rows), rows)

    def g_cols(d):
        return g_hbm.at[:, pl.ds(pl.multiple_of(d * cols, cols), cols)]

    locals_ = [
        pltpu.make_async_copy(g_cols(across), kv.at[0, my_rows, :], local_sem.at[0]),
        pltpu.make_async_copy(g_cols(dp), kv.at[2, my_rows, :], local_sem.at[1]),
        pltpu.make_async_copy(a_hbm, a_buf, local_sem.at[2]),
        pltpu.make_async_copy(b_hbm, b_buf, local_sem.at[3]),
        pltpu.make_async_copy(x_hbm, xs.at[0], local_sem.at[4]),
        pltpu.make_async_copy(m_hbm, m_buf, local_sem.at[5]),
        pltpu.make_async_copy(v_hbm, v_buf, local_sem.at[6]),
    ]
    for copy in locals_:
        copy.start()

    barrier = pltpu.get_barrier_semaphore()

    def hello(where):
        pl.semaphore_signal(barrier, inc=1, device_id=where, device_id_type=pl.DeviceIdType.MESH)

    hello({"dp": beside})
    hello({"dp": across})
    hello({"tp": other})

    @pl.when(z + 1 < n_z)
    def _():
        hello({"tp": tp + 2})

    pl.semaphore_wait(barrier, 3 + jnp.where(z >= 1, 1, 0))

    @pl.when(z >= 1)
    def _():
        pl.semaphore_signal(upper_in, inc=1, device_id={"tp": tp - 2}, device_id_type=pl.DeviceIdType.MESH)

    def swap(i, plane, d):
        return remote(g_cols(d), kv.at[plane, my_rows, :], swap_send.at[i], swap_recv.at[i], {"dp": beside})

    swaps = [swap(0, 1, jnp.bitwise_xor(dp, 3)), swap(1, 3, beside)]

    def x_copy(k):
        at = pl.ds(k * LANES, LANES)
        return remote(x_hbm.at[:, at], xs.at[1, :, at], x_send.at[k], x_recv.at[k], {"dp": beside})

    go(swaps[0])
    go(swaps[1])
    for k in range(EARLY):
        go(x_copy(k))

    GAIN = 4

    def block(g, b, c):
        if g == GAIN:
            return gain_z.at[b]
        return kv.at[g, pl.ds(pl.multiple_of((2 * b + c) * rows, rows), rows), :]

    def to_pair(g, b):
        return remote(block(g, b, core), block(g, b, core), pair_send.at[g, b], pair_recv.at[g, b], {"tp": other})

    def from_pair(g, b):
        return remote(block(g, b, 1 - core), block(g, b, 1 - core), pair_send.at[g, b], pair_recv.at[g, b], {"tp": other})

    def up(g, s):
        b = z - s + 1
        return remote(block(g, b, core), block(g, b, core), up_send.at[g, s], up_recv.at[g, s], {"tp": tp + 2})

    def down(g, s):
        b = z + s - 1
        return remote(block(g, b, core), block(g, b, core), down_send.at[g, s], down_recv.at[g, s], {"tp": tp - 2})

    def up_got(g, s):
        b = z - s
        return remote(block(g, b, core), block(g, b, core), up_send.at[g, s], up_recv.at[g, s], {"tp": other})

    def down_got(g, s):
        b = z + s
        return remote(block(g, b, core), block(g, b, core), down_send.at[g, s], down_recv.at[g, s], {"tp": other})

    def chain(g, s):
        if s > 1:
            @pl.when(z - s + 1 >= 0)
            def _():
                up_got(g, s - 1).wait_recv()

        if s < n_z:
            @pl.when((z - s + 1 >= 0) & (z + 1 < n_z))
            def _():
                up(g, s).start()

        if s > 1:
            @pl.when(z + s - 1 < n_z)
            def _():
                down_got(g, s - 1).wait_recv()

        if s < n_z:
            @pl.when((z + s - 1 < n_z) & (z - 1 >= 0))
            def _():
                down(g, s).start()

        if g == GAIN:
            return
        if s == 1:
            to_pair(g, z).start()
        else:
            @pl.when(z - s + 1 >= 0)
            def _():
                to_pair(g, z - s + 1).start()

            @pl.when(z + s - 1 < n_z)
            def _():
                to_pair(g, z + s - 1).start()

    def complete(g):
        for b in range(n_z):
            from_pair(g, b).wait_recv()

    def gain_copy(i, src, dst, where):
        return remote(src, dst, gain_send.at[i], gain_recv.at[i], where)

    def dot(x, w):
        return lax.dot_general(x, w, (((0,), (0,)), ((), ())), preferred_element_type=jnp.float32)

    halves = 2
    wide = cols // halves

    def part_copy(k, h):
        at = (k, slice(None), pl.ds(h * wide, wide))
        return remote(part.at[at], arrived.at[at], part_send.at[k, h], part_recv.at[k, h], {"dp": across})

    def partial(k):
        at = pl.ds(k * LANES, LANES)
        last = k == chunks - 1
        if last:
            ready[...] = dot(xs[0, :, at], kv[0])
        x_copy(k).wait_recv()
        for h in range(halves):
            ch = pl.ds(h * wide, wide)
            head = ready[:, ch] if last else dot(xs[0, :, at], kv[0, :, ch])
            total = head + dot(xs[1, :, at], kv[1, :, ch])
            held = jnp.max(jnp.abs(total), axis=0, keepdims=True).astype(jnp.bfloat16)
            part[k, pl.ds(LANES, NOTE), ch] = jnp.broadcast_to(held, (NOTE, wide))
            part[k, pl.ds(0, LANES), ch] = encode(total, scale_of(held))
            go(part_copy(k, h))

    def own_sum(k):
        at = pl.ds(k * LANES, LANES)
        own[at, :] = dot(xs[0, :, at], kv[2]) + dot(xs[1, :, at], kv[3])

    def finish(k):
        at = pl.ds(k * LANES, LANES)
        for h in range(halves):
            ch = pl.ds(h * wide, wide)
            part_copy(k, h).wait_recv()
            scale = scale_of(arrived[k, pl.ds(LANES, NOTE), ch][:1])
            mean = (own[at, ch] + decode(arrived[k, pl.ds(0, LANES), ch], scale)) / n_dp
            new_first, new_second, update = adam_update(mean, m_buf[at, ch], v_buf[at, ch])
            first_ref[at, ch] = new_first
            second_ref[at, ch] = new_second
            step_ref[at, ch] = update

    @pl.when(z + 1 < n_z)
    def _():
        pl.semaphore_wait(upper_in, 1)

    locals_[0].wait()
    chain(0, 1)
    locals_[1].wait()
    chain(2, 1)

    locals_[2].wait()
    locals_[3].wait()
    lines, span = gain_half.shape[1:]
    for h in range(2):
        for j in range(lines):
            at = pl.ds((h * lines + j) * span, span)
            products = a_buf[:, at].astype(jnp.float32) * b_buf[:, at].astype(jnp.float32)
            gain_half[h, pl.ds(j, 1), :] = jnp.sum(products, axis=0, keepdims=True)
    pair_gain = gain_copy(0, gain_half.at[1 - core], gain_pair.at[1], {"tp": other})
    beside_gain = gain_copy(1, gain_x.at[0], gain_x.at[1], {"dp": beside})
    across_gain = gain_copy(2, gain_y.at[0], gain_y.at[1], {"dp": across})
    go(pair_gain)
    swaps[0].wait_recv()
    chain(1, 1)
    pair_gain.wait_recv()
    gain_x[0] = gain_half[core] + gain_pair[1]
    go(beside_gain)
    for k in range(EARLY, chunks):
        go(x_copy(k))
    chain(0, 2)
    swaps[1].wait_recv()
    chain(1, 2)
    chain(0, 3)
    chain(1, 3)
    chain(3, 1)
    chain(2, 2)
    for s in range(4, n_z + 1):
        chain(0, s)
        chain(1, s)
    complete(0)
    complete(1)
    locals_[4].wait()

    partial(0)
    chain(3, 2)
    partial(1)
    chain(2, 3)
    beside_gain.wait_recv()
    gain_y[0] = gain_x[0] + gain_x[1]
    go(across_gain)
    chain(3, 3)
    partial(2)
    across_gain.wait_recv()
    gain_z[z] = gain_y[0] + gain_y[1]
    chain(GAIN, 1)
    partial(3)
    for s in range(4, n_z + 1):
        chain(2, s)
    partial(4)
    for s in range(4, n_z + 1):
        chain(3, s)
    chain(GAIN, 2)
    complete(2)
    complete(3)
    for copy in locals_[5:]:
        copy.wait()
    for k in range(3):
        own_sum(k)
    for k in range(2):
        finish(k)
    partial(5)
    chain(GAIN, 3)
    for k in range(3, 6):
        own_sum(k)
    for k in range(2, 5):
        finish(k)
    partial(6)
    for s in range(4, n_z + 1):
        chain(GAIN, s)
    gain_all[core] = jnp.sum(gain_z[...], axis=0) / n_dp
    last_gain = gain_copy(3, gain_all.at[core], gain_all.at[core], {"tp": other})
    go(last_gain)
    own_sum(6)
    finish(5)
    gain_copy(3, gain_all.at[1 - core], gain_all.at[1 - core], {"tp": other}).wait_recv()
    per = span // LANES
    for h in range(2):
        for i in range(per):
            at = pl.ds(h * lines * per + i, lines, stride=per)
            gain_ref[at, :] = gain_all[h, :, i * LANES:(i + 1) * LANES]
    finish(6)
    for k in range(7, chunks):
        partial(k)
    for k in range(7, chunks):
        own_sum(k)
    for k in range(7, chunks):
        finish(k)

    for copy in sent:
        copy.wait_send()
    for g in range(GAIN + 1):
        for s in range(1, n_z):
            @pl.when((z - s + 1 >= 0) & (z + 1 < n_z))
            def _():
                up(g, s).wait_send()

            @pl.when((z + s - 1 < n_z) & (z - 1 >= 0))
            def _():
                down(g, s).wait_send()
        if g < GAIN:
            for b in range(n_z):
                to_pair(g, b).wait_send()


def store_kernel(*refs):
    count = (len(refs) - 1) // 2
    copies = [pltpu.make_async_copy(refs[i], refs[count + i], refs[-1].at[i]) for i in range(count)]
    for copy in copies:
        copy.start()
    for copy in copies:
        copy.wait()


def store_call(*arrays):
    return pl.pallas_call(
        store_kernel,
        out_shape=tuple(jax.ShapeDtypeStruct(a.shape, a.dtype) for a in arrays),
        in_specs=[pl.BlockSpec(memory_space=pltpu.VMEM)] * len(arrays),
        out_specs=(pl.BlockSpec(memory_space=pltpu.HBM),) * len(arrays),
        scratch_shapes=[pltpu.SemaphoreType.DMA((len(arrays),))],
        compiler_params=pltpu.CompilerParams(vmem_limit_bytes=1024 * 1024),
    )(*arrays)


def pair_call(layer, n_tp, x, g, a, b, m, v):
    tokens, features = x.shape
    rows, width = g.shape
    model = a.shape[1]
    n_dp = 4
    cols = width // n_dp
    n_z = n_tp // 2
    chunks = features // LANES
    span = model // 16
    dma = pltpu.SemaphoreType.DMA
    bf16, f32 = jnp.bfloat16, jnp.float32
    buffers = [
        ((2, tokens, features), bf16), ((4, tokens, cols), bf16),
        ((chunks, LANES + NOTE, cols), bf16), ((chunks, LANES + NOTE, cols), bf16), ((features, cols), f32),
        ((features, cols), f32), ((features, cols), f32),
        ((rows, model), bf16), ((rows, model), bf16),
        ((2, 8, span), f32), ((2, 8, span), f32), ((2, 8, span), f32), ((2, 8, span), f32),
        ((n_z, 8, span), f32), ((2, 8, span), f32),
    ]
    total = jax.ShapeDtypeStruct((features, cols), f32)
    return pl.pallas_call(
        functools.partial(pair_kernel, n_tp),
        out_shape=(total, total, total, jax.ShapeDtypeStruct((model // LANES, LANES), f32)),
        in_specs=[pl.BlockSpec(memory_space=pltpu.HBM)] * 6,
        out_specs=(pl.BlockSpec(memory_space=pltpu.VMEM),) * 4,
        scratch_shapes=[pltpu.VMEM(shape, dtype) for shape, dtype in buffers] + [
            dma((7,)), dma((2,)), dma((2,)), dma((chunks,)), dma((chunks,)), dma((chunks, 2)), dma((chunks, 2)),
        ] + [dma((5, n_z))] * 6 + [dma((4,)), dma((4,)), pltpu.SemaphoreType.REGULAR, pltpu.VMEM((LANES, cols), f32)],
        compiler_params=pltpu.CompilerParams(
            collective_id=layer, has_side_effects=True, vmem_limit_bytes=VMEM_LIMIT,
        ),
    )(x, g, a, b, m, v)


def shards(n_dp, n_tp, proj_in, kv_grad, normed, norm_grad, first_moment, second_moment):
    layers, tokens, features = proj_in.shape
    rows, width = kv_grad.shape[1:]
    model = normed.shape[2]
    cols = width // n_dp
    lines = 8
    dma = pltpu.SemaphoreType.DMA
    n_z = n_tp // 2
    firsts, seconds, updates, gains = [], [], [], []
    for layer in range(layers):
        if n_dp == 4 and features % LANES == 0 and features >= 8 * LANES and model % (16 * LANES) == 0 and n_tp >= 6:
            new_first, new_second, update, gain = store_call(*pair_call(
                layer, n_tp, proj_in[layer], pltpu.with_memory_space_constraint(kv_grad[layer], pltpu.HBM), normed[layer], norm_grad[layer],
                first_moment[layer], second_moment[layer],
            ))
        else:
            total, gain = pl.pallas_call(
                functools.partial(kernel, n_dp, n_tp),
                out_shape=(
                    jax.ShapeDtypeStruct((features, cols), jnp.float32),
                    jax.ShapeDtypeStruct((lines, model // lines), jnp.float32),
                ),
                in_specs=[pl.BlockSpec(memory_space=pltpu.HBM)] * 4,
                out_specs=(pl.BlockSpec(memory_space=pltpu.VMEM), pl.BlockSpec(memory_space=pltpu.VMEM)),
                scratch_shapes=[
                    pltpu.VMEM((n_dp, tokens, features), jnp.bfloat16),
                    pltpu.VMEM((n_dp, n_tp * rows, cols), jnp.bfloat16),
                    pltpu.VMEM((rows, model), jnp.bfloat16),
                    pltpu.VMEM((rows, model), jnp.bfloat16),
                    pltpu.VMEM((n_tp, lines, model // lines), jnp.float32),
                    pltpu.VMEM((n_dp, lines, model // lines), jnp.float32),
                    dma((4,)),
                    dma((n_dp, PIECES)), dma((n_dp, PIECES)),
                    dma((n_dp,)), dma((n_dp,)),
                    dma((n_z,)), dma((n_z,)), dma((n_z,)), dma((n_z,)),
                    dma((n_z,)), dma((n_z,)),
                    dma((n_tp,)), dma((n_tp,)), dma((n_dp,)), dma((n_dp,)),
                ],
                compiler_params=pltpu.CompilerParams(
                    collective_id=layer, has_side_effects=True, vmem_limit_bytes=60 * 1024 * 1024,
                ),
            )(proj_in[layer], kv_grad[layer], normed[layer], norm_grad[layer])
            new_first, new_second, update = adam_update(total / n_dp, first_moment[layer], second_moment[layer])
        firsts.append(new_first)
        seconds.append(new_second)
        updates.append(update)
        gains.append(gain.reshape(model))
    return (jnp.stack(firsts), jnp.stack(seconds), jnp.stack(updates), jnp.stack(gains))


def solution(mesh):
    return jax.shard_map(
        functools.partial(shards, mesh.shape["dp"], mesh.shape["tp"]),
        mesh=mesh,
        in_specs=(
            P(None, "dp", "tp"),
            P(None, ("dp", "tp"), None),
            P(None, ("dp", "tp"), None),
            P(None, ("dp", "tp"), None),
            P(None, "tp", "dp"),
            P(None, "tp", "dp"),
        ),
        out_specs=(P(None, "tp", "dp"), P(None, "tp", "dp"), P(None, "tp", "dp"), P()),
        check_vma=False,
    )
```

```python
import functools
import math

import jax
import jax.numpy as jnp
from jax import lax
from jax.experimental import pallas as pl
from jax.experimental.pallas import tpu as pltpu
from jax.sharding import PartitionSpec as P

beta_one = 0.9
beta_two = 0.95
correct_one = 0.19
correct_two = 0.0975
epsilon = 1e-08
PIECES = 4
LANES = 128
SPAN = 250.0
KNEE = 2.0 ** -10
POWER = SPAN / math.log2(1.0 + 1.0 / KNEE)
TINY = 2.0 ** -100
NOTE = 16
EARLY = 2
VMEM_LIMIT = 46 * 1024 * 1024


def adam_update(mean_grad, first_old, second_old):
    new_first = beta_one * first_old + (1.0 - beta_one) * mean_grad
    new_second = beta_two * second_old + (1.0 - beta_two) * mean_grad * mean_grad
    update = new_first / correct_one / (jnp.sqrt(new_second / correct_two) + epsilon)
    return (new_first, new_second, update)


def kernel(
    n_dp, n_tp, x_hbm, g_hbm, a_hbm, b_hbm, sum_ref, gain_ref,
    xs, kv, a_buf, b_buf, gain_tp, gain_dp,
    local_sem, x_send, x_recv, a2a_send, a2a_recv,
    up_send, up_recv, down_send, down_recv, pair_send, pair_recv,
    gt_send, gt_recv, gd_send, gd_recv,
):
    dp = lax.axis_index("dp")
    tp = lax.axis_index("tp")
    z = tp // 2
    core = tp % 2
    n_z = n_tp // 2
    rows = g_hbm.shape[0]
    cols = kv.shape[2]
    tokens = x_hbm.shape[0]
    piece = tokens // PIECES

    def dp_peer(o):
        return jnp.bitwise_xor(dp, o)

    def tp_peer(o):
        return lax.rem(tp + o, n_tp)

    locals_ = [
        pltpu.make_async_copy(a_hbm, a_buf, local_sem.at[0]),
        pltpu.make_async_copy(b_hbm, b_buf, local_sem.at[1]),
        pltpu.make_async_copy(
            g_hbm.at[:, pl.ds(pl.multiple_of(dp * cols, cols), cols)],
            kv.at[dp, pl.ds(pl.multiple_of(tp * rows, rows), rows), :],
            local_sem.at[2],
        ),
        pltpu.make_async_copy(x_hbm, xs.at[dp], local_sem.at[3]),
    ]
    for copy in locals_:
        copy.start()

    barrier = pltpu.get_barrier_semaphore()
    for o in range(1, n_dp):
        pl.semaphore_signal(barrier, inc=1, device_id={"dp": dp_peer(o)}, device_id_type=pl.DeviceIdType.MESH)
    for o in range(1, n_tp):
        pl.semaphore_signal(barrier, inc=1, device_id={"tp": tp_peer(o)}, device_id_type=pl.DeviceIdType.MESH)
    pl.semaphore_wait(barrier, n_dp - 1 + n_tp - 1)

    sent = []

    def remote(src, dst, send, recv, where):
        return pltpu.make_async_remote_copy(
            src_ref=src, dst_ref=dst, send_sem=send, recv_sem=recv,
            device_id=where, device_id_type=pl.DeviceIdType.MESH,
        )

    my_rows = pl.ds(pl.multiple_of(tp * rows, rows), rows)
    a2a = []
    for o in range(1, n_dp):
        peer = dp_peer(o)
        copy = remote(
            g_hbm.at[:, pl.ds(pl.multiple_of(peer * cols, cols), cols)],
            kv.at[dp, my_rows, :], a2a_send.at[o], a2a_recv.at[o], {"dp": peer},
        )
        copy.start()
        a2a.append(copy)
        sent.append(copy)

    def x_copy(src, origin, c, o_recv, o_to, send):
        part = pl.ds(c * piece, piece)
        return remote(
            src.at[part, :], xs.at[origin, part, :], send, x_recv.at[o_recv, c],
            {"dp": dp_peer(o_to)},
        )

    square = n_dp == 4
    orders = {o: list(range(PIECES)) for o in range(1, n_dp)}
    half = PIECES // 2
    if square:
        orders[2] = list(range(half, PIECES)) + list(range(half))
        orders[3] = []

    def send_own(i):
        for o in range(1, n_dp):
            if i < len(orders[o]):
                c = orders[o][i]
                copy = x_copy(x_hbm, dp, c, o, o, x_send.at[o, c])
                copy.start()
                sent.append(copy)

    def got(o, c):
        x_copy(xs.at[dp_peer(o)], dp_peer(o), c, o, o, x_send.at[o, c]).wait_recv()

    def forward(i):
        for o, o_to in ((1, 2), (2, 1)):
            c = orders[o][i]
            got(o, c)
            copy = x_copy(xs.at[dp_peer(o)], dp_peer(o), c, 3, o_to, x_send.at[3, c])
            copy.start()
            sent.append(copy)

    send_own(0)
    send_own(1)

    locals_[0].wait()
    locals_[1].wait()
    wide = gain_tp.shape[2]
    lines = gain_tp.shape[1]
    for j in range(lines):
        s = pl.ds(j * wide, wide)
        products = a_buf[:, s].astype(jnp.float32) * b_buf[:, s].astype(jnp.float32)
        gain_tp[tp, pl.ds(j, 1), :] = jnp.sum(products, axis=0, keepdims=True)
    tp_copies = []
    for o in range(1, n_tp):
        copy = remote(gain_tp.at[tp], gain_tp.at[tp], gt_send.at[o], gt_recv.at[o], {"tp": tp_peer(o)})
        copy.start()
        sent.append(copy)
        tp_copies.append(copy)

    def block(b, c):
        return kv.at[:, pl.ds(pl.multiple_of((2 * b + c) * rows, rows), rows), :]

    other = 2 * z + 1 - core

    def to_pair(b):
        return remote(block(b, core), block(b, core), pair_send.at[b], pair_recv.at[b], {"tp": other})

    def up(s):
        b = z - s + 1
        return remote(block(b, core), block(b, core), up_send.at[s], up_recv.at[s], {"tp": tp + 2})

    def down(s):
        b = z + s - 1
        return remote(block(b, core), block(b, core), down_send.at[s], down_recv.at[s], {"tp": tp - 2})

    def up_got(s):
        b = z - s
        return remote(block(b, core), block(b, core), up_send.at[s], up_recv.at[s], {"tp": other})

    def down_got(s):
        b = z + s
        return remote(block(b, core), block(b, core), down_send.at[s], down_recv.at[s], {"tp": other})

    locals_[2].wait()
    for o in range(1, n_dp):
        a2a[o - 1].wait_recv()

    for s in range(1, n_z + 1):
        if s > 1:
            @pl.when(z - s + 1 >= 0)
            def _():
                up_got(s - 1).wait_recv()

        if s < n_z:
            @pl.when((z - s + 1 >= 0) & (z + 1 < n_z))
            def _():
                up(s).start()

        if s > 1:
            @pl.when(z + s - 1 < n_z)
            def _():
                down_got(s - 1).wait_recv()

        if s < n_z:
            @pl.when((z + s - 1 < n_z) & (z - 1 >= 0))
            def _():
                down(s).start()

        if s == 1:
            to_pair(z).start()
        else:
            @pl.when(z - s + 1 >= 0)
            def _():
                to_pair(z - s + 1).start()

            @pl.when(z + s - 1 < n_z)
            def _():
                to_pair(z + s - 1).start()

        if s == 1:
            for copy in tp_copies:
                copy.wait_recv()
            gain_dp[dp, :, :] = jnp.sum(gain_tp[...], axis=0)
            for o in range(1, n_dp):
                copy = remote(gain_dp.at[dp], gain_dp.at[dp], gd_send.at[o], gd_recv.at[o], {"dp": dp_peer(o)})
                copy.start()
                sent.append(copy)
            for i in range(2, PIECES):
                send_own(i)
        if square and 2 <= s < 2 + half:
            forward(s - 2)
    if square:
        for i in range(max(n_z - 1, 0), half):
            forward(i)

    for b in range(n_z):
        remote(block(b, 1 - core), block(b, 1 - core), pair_send.at[b], pair_recv.at[b], {"tp": other}).wait_recv()

    width = min(256, sum_ref.shape[0])

    def multiply(origin, start, size, first=False):
        @pl.loop(0, sum_ref.shape[0] // width)
        def _(f):
            at = pl.ds(pl.multiple_of(f * width, width), width)
            part = lax.dot_general(
                xs[origin, pl.ds(start, size), at], kv[origin, pl.ds(start, size), :],
                (((0,), (0,)), ((), ())), preferred_element_type=jnp.float32,
            )
            if first:
                sum_ref[at, :] = part
            else:
                sum_ref[at, :] += part

    locals_[3].wait()
    multiply(dp, 0, tokens, True)
    for o in range(1, n_dp):
        if square and o == 3:
            continue
        for c in orders[o]:
            if not (square and c in orders[o][:half]):
                got(o, c)
        multiply(dp_peer(o), 0, tokens)

    for o in range(1, n_dp):
        remote(gain_dp.at[dp_peer(o)], gain_dp.at[dp_peer(o)], gd_send.at[o], gd_recv.at[o], {"dp": dp_peer(o)}).wait_recv()
    gain_ref[...] = jnp.sum(gain_dp[...], axis=0) / n_dp

    if square:
        for i in range(half):
            for o in (1, 2):
                c = orders[o][i]
                got(3, c)
                multiply(dp_peer(3), c * piece, piece)

    for copy in sent:
        copy.wait_send()
    for s in range(1, n_z):
        @pl.when((z - s + 1 >= 0) & (z + 1 < n_z))
        def _():
            up(s).wait_send()

        @pl.when((z + s - 1 < n_z) & (z - 1 >= 0))
        def _():
            down(s).wait_send()
    for b in range(n_z):
        to_pair(b).wait_send()


def scale_of(held):
    return jnp.maximum(held.astype(jnp.float32), TINY)


def encode(value, scale):
    code = jnp.exp2(POWER * jnp.log2(1.0 + jnp.abs(value) * (1.0 / (scale * KNEE))) - SPAN / 2)
    return jnp.where(value < 0.0, -code, code).astype(jnp.bfloat16)


def decode(code, scale):
    code = code.astype(jnp.float32)
    value = (jnp.exp2((jnp.log2(jnp.abs(code)) + SPAN / 2) * (1.0 / POWER)) - 1.0) * (scale * KNEE)
    return jnp.where(code < 0.0, -value, value)


def pair_kernel(
    n_tp, x_hbm, g_hbm, a_hbm, b_hbm, m_hbm, v_hbm, first_ref, second_ref, step_ref, gain_ref,
    xs, kv, part, arrived, own, m_buf, v_buf, a_buf, b_buf, gain_half, gain_pair, gain_x, gain_y, gain_z, gain_all,
    local_sem, swap_send, swap_recv, x_send, x_recv, part_send, part_recv,
    up_send, up_recv, down_send, down_recv, pair_send, pair_recv, gain_send, gain_recv, upper_in, ready,
):
    n_dp = 4
    dp = lax.axis_index("dp")
    tp = lax.axis_index("tp")
    z = tp // 2
    core = tp % 2
    n_z = n_tp // 2
    rows = g_hbm.shape[0]
    cols = kv.shape[2]
    tokens, features = x_hbm.shape
    chunks = features // LANES
    other = 2 * z + 1 - core
    beside = jnp.bitwise_xor(dp, 1)
    across = jnp.bitwise_xor(dp, 2)
    sent = []

    def remote(src, dst, send, recv, where):
        return pltpu.make_async_remote_copy(
            src_ref=src, dst_ref=dst, send_sem=send, recv_sem=recv,
            device_id=where, device_id_type=pl.DeviceIdType.MESH,
        )

    def go(copy):
        copy.start()
        sent.append(copy)

    my_rows = pl.ds(pl.multiple_of(tp * rows, rows), rows)

    def g_cols(d):
        return g_hbm.at[:, pl.ds(pl.multiple_of(d * cols, cols), cols)]

    locals_ = [
        pltpu.make_async_copy(g_cols(across), kv.at[0, my_rows, :], local_sem.at[0]),
        pltpu.make_async_copy(g_cols(dp), kv.at[2, my_rows, :], local_sem.at[1]),
        pltpu.make_async_copy(a_hbm, a_buf, local_sem.at[2]),
        pltpu.make_async_copy(b_hbm, b_buf, local_sem.at[3]),
        pltpu.make_async_copy(x_hbm, xs.at[0], local_sem.at[4]),
        pltpu.make_async_copy(m_hbm, m_buf, local_sem.at[5]),
        pltpu.make_async_copy(v_hbm, v_buf, local_sem.at[6]),
    ]
    for copy in locals_:
        copy.start()

    barrier = pltpu.get_barrier_semaphore()

    def hello(where):
        pl.semaphore_signal(barrier, inc=1, device_id=where, device_id_type=pl.DeviceIdType.MESH)

    hello({"dp": beside})
    hello({"dp": across})
    hello({"tp": other})

    @pl.when(z + 1 < n_z)
    def _():
        hello({"tp": tp + 2})

    pl.semaphore_wait(barrier, 3 + jnp.where(z >= 1, 1, 0))

    @pl.when(z >= 1)
    def _():
        pl.semaphore_signal(upper_in, inc=1, device_id={"tp": tp - 2}, device_id_type=pl.DeviceIdType.MESH)

    def swap(i, plane, d):
        return remote(g_cols(d), kv.at[plane, my_rows, :], swap_send.at[i], swap_recv.at[i], {"dp": beside})

    swaps = [swap(0, 1, jnp.bitwise_xor(dp, 3)), swap(1, 3, beside)]

    def x_copy(k):
        at = pl.ds(k * LANES, LANES)
        return remote(x_hbm.at[:, at], xs.at[1, :, at], x_send.at[k], x_recv.at[k], {"dp": beside})

    go(swaps[0])
    go(swaps[1])
    for k in range(EARLY):
        go(x_copy(k))

    GAIN = 4

    def block(g, b, c):
        if g == GAIN:
            return gain_z.at[b]
        return kv.at[g, pl.ds(pl.multiple_of((2 * b + c) * rows, rows), rows), :]

    def to_pair(g, b):
        return remote(block(g, b, core), block(g, b, core), pair_send.at[g, b], pair_recv.at[g, b], {"tp": other})

    def from_pair(g, b):
        return remote(block(g, b, 1 - core), block(g, b, 1 - core), pair_send.at[g, b], pair_recv.at[g, b], {"tp": other})

    def up(g, s):
        b = z - s + 1
        return remote(block(g, b, core), block(g, b, core), up_send.at[g, s], up_recv.at[g, s], {"tp": tp + 2})

    def down(g, s):
        b = z + s - 1
        return remote(block(g, b, core), block(g, b, core), down_send.at[g, s], down_recv.at[g, s], {"tp": tp - 2})

    def up_got(g, s):
        b = z - s
        return remote(block(g, b, core), block(g, b, core), up_send.at[g, s], up_recv.at[g, s], {"tp": other})

    def down_got(g, s):
        b = z + s
        return remote(block(g, b, core), block(g, b, core), down_send.at[g, s], down_recv.at[g, s], {"tp": other})

    def chain(g, s):
        if s > 1:
            @pl.when(z - s + 1 >= 0)
            def _():
                up_got(g, s - 1).wait_recv()

        if s < n_z:
            @pl.when((z - s + 1 >= 0) & (z + 1 < n_z))
            def _():
                up(g, s).start()

        if s > 1:
            @pl.when(z + s - 1 < n_z)
            def _():
                down_got(g, s - 1).wait_recv()

        if s < n_z:
            @pl.when((z + s - 1 < n_z) & (z - 1 >= 0))
            def _():
                down(g, s).start()

        if g == GAIN:
            return
        if s == 1:
            to_pair(g, z).start()
        else:
            @pl.when(z - s + 1 >= 0)
            def _():
                to_pair(g, z - s + 1).start()

            @pl.when(z + s - 1 < n_z)
            def _():
                to_pair(g, z + s - 1).start()

    def complete(g):
        for b in range(n_z):
            from_pair(g, b).wait_recv()

    def gain_copy(i, src, dst, where):
        return remote(src, dst, gain_send.at[i], gain_recv.at[i], where)

    def dot(x, w):
        return lax.dot_general(x, w, (((0,), (0,)), ((), ())), preferred_element_type=jnp.float32)

    halves = 2
    wide = cols // halves

    def part_copy(k, h):
        at = (k, slice(None), pl.ds(h * wide, wide))
        return remote(part.at[at], arrived.at[at], part_send.at[k, h], part_recv.at[k, h], {"dp": across})

    def partial(k):
        at = pl.ds(k * LANES, LANES)
        last = k == chunks - 1
        if last:
            ready[...] = dot(xs[0, :, at], kv[0])
        x_copy(k).wait_recv()
        for h in range(halves):
            ch = pl.ds(h * wide, wide)
            head = ready[:, ch] if last else dot(xs[0, :, at], kv[0, :, ch])
            total = head + dot(xs[1, :, at], kv[1, :, ch])
            held = jnp.max(jnp.abs(total), axis=0, keepdims=True).astype(jnp.bfloat16)
            part[k, pl.ds(LANES, NOTE), ch] = jnp.broadcast_to(held, (NOTE, wide))
            part[k, pl.ds(0, LANES), ch] = encode(total, scale_of(held))
            go(part_copy(k, h))

    def own_sum(k):
        at = pl.ds(k * LANES, LANES)
        own[at, :] = dot(xs[0, :, at], kv[2]) + dot(xs[1, :, at], kv[3])

    def finish(k):
        at = pl.ds(k * LANES, LANES)
        for h in range(halves):
            ch = pl.ds(h * wide, wide)
            part_copy(k, h).wait_recv()
            scale = scale_of(arrived[k, pl.ds(LANES, NOTE), ch][:1])
            mean = (own[at, ch] + decode(arrived[k, pl.ds(0, LANES), ch], scale)) / n_dp
            new_first, new_second, update = adam_update(mean, m_buf[at, ch], v_buf[at, ch])
            first_ref[at, ch] = new_first
            second_ref[at, ch] = new_second
            step_ref[at, ch] = update

    @pl.when(z + 1 < n_z)
    def _():
        pl.semaphore_wait(upper_in, 1)

    locals_[0].wait()
    chain(0, 1)
    locals_[1].wait()
    chain(2, 1)

    locals_[2].wait()
    locals_[3].wait()
    lines, span = gain_half.shape[1:]
    for h in range(2):
        for j in range(lines):
            at = pl.ds((h * lines + j) * span, span)
            products = a_buf[:, at].astype(jnp.float32) * b_buf[:, at].astype(jnp.float32)
            gain_half[h, pl.ds(j, 1), :] = jnp.sum(products, axis=0, keepdims=True)
    pair_gain = gain_copy(0, gain_half.at[1 - core], gain_pair.at[1], {"tp": other})
    beside_gain = gain_copy(1, gain_x.at[0], gain_x.at[1], {"dp": beside})
    across_gain = gain_copy(2, gain_y.at[0], gain_y.at[1], {"dp": across})
    go(pair_gain)
    swaps[0].wait_recv()
    chain(1, 1)
    pair_gain.wait_recv()
    gain_y[0] = gain_half[core] + gain_pair[1]
    go(across_gain)
    for k in range(EARLY, chunks):
        go(x_copy(k))
    chain(0, 2)
    swaps[1].wait_recv()
    chain(1, 2)
    chain(0, 3)
    chain(1, 3)
    chain(3, 1)
    chain(2, 2)
    for s in range(4, n_z + 1):
        chain(0, s)
        chain(1, s)
    complete(0)
    complete(1)
    locals_[4].wait()

    partial(0)
    chain(3, 2)
    partial(1)
    chain(2, 3)
    chain(3, 3)
    partial(2)
    across_gain.wait_recv()
    gain_z[z] = gain_y[0] + gain_y[1]
    chain(GAIN, 1)
    partial(3)
    for s in range(4, n_z + 1):
        chain(2, s)
    partial(4)
    for s in range(4, n_z + 1):
        chain(3, s)
    chain(GAIN, 2)
    complete(2)
    complete(3)
    for copy in locals_[5:]:
        copy.wait()
    for k in range(3):
        own_sum(k)
    for k in range(2):
        finish(k)
    partial(5)
    chain(GAIN, 3)
    for k in range(3, 6):
        own_sum(k)
    for k in range(2, 5):
        finish(k)
    partial(6)
    for s in range(4, n_z + 1):
        chain(GAIN, s)
    gain_x[0] = jnp.sum(gain_z[...], axis=0)
    go(beside_gain)
    own_sum(6)
    finish(5)
    finish(6)
    for k in range(7, chunks):
        partial(k)
    for k in range(7, chunks):
        own_sum(k)
    beside_gain.wait_recv()
    gain_all[core] = (gain_x[0] + gain_x[1]) / n_dp
    go(gain_copy(3, gain_all.at[core], gain_all.at[core], {"tp": other}))
    gain_copy(3, gain_all.at[1 - core], gain_all.at[1 - core], {"tp": other}).wait_recv()
    per = span // LANES
    for h in range(2):
        for i in range(per):
            at = pl.ds(h * lines * per + i, lines, stride=per)
            gain_ref[at, :] = gain_all[h, :, i * LANES:(i + 1) * LANES]
    for k in range(7, chunks):
        finish(k)

    for copy in sent:
        copy.wait_send()
    for g in range(GAIN + 1):
        for s in range(1, n_z):
            @pl.when((z - s + 1 >= 0) & (z + 1 < n_z))
            def _():
                up(g, s).wait_send()

            @pl.when((z + s - 1 < n_z) & (z - 1 >= 0))
            def _():
                down(g, s).wait_send()
        if g < GAIN:
            for b in range(n_z):
                to_pair(g, b).wait_send()


def store_kernel(*refs):
    count = (len(refs) - 1) // 2
    copies = [pltpu.make_async_copy(refs[i], refs[count + i], refs[-1].at[i]) for i in range(count)]
    for copy in copies:
        copy.start()
    for copy in copies:
        copy.wait()


def store_call(*arrays):
    return pl.pallas_call(
        store_kernel,
        out_shape=tuple(jax.ShapeDtypeStruct(a.shape, a.dtype) for a in arrays),
        in_specs=[pl.BlockSpec(memory_space=pltpu.VMEM)] * len(arrays),
        out_specs=(pl.BlockSpec(memory_space=pltpu.HBM),) * len(arrays),
        scratch_shapes=[pltpu.SemaphoreType.DMA((len(arrays),))],
        compiler_params=pltpu.CompilerParams(vmem_limit_bytes=1024 * 1024),
    )(*arrays)


def pair_call(layer, n_tp, x, g, a, b, m, v):
    tokens, features = x.shape
    rows, width = g.shape
    model = a.shape[1]
    n_dp = 4
    cols = width // n_dp
    n_z = n_tp // 2
    chunks = features // LANES
    span = model // 16
    dma = pltpu.SemaphoreType.DMA
    bf16, f32 = jnp.bfloat16, jnp.float32
    buffers = [
        ((2, tokens, features), bf16), ((4, tokens, cols), bf16),
        ((chunks, LANES + NOTE, cols), bf16), ((chunks, LANES + NOTE, cols), bf16), ((features, cols), f32),
        ((features, cols), f32), ((features, cols), f32),
        ((rows, model), bf16), ((rows, model), bf16),
        ((2, 8, span), f32), ((2, 8, span), f32), ((2, 8, span), f32), ((2, 8, span), f32),
        ((n_z, 8, span), f32), ((2, 8, span), f32),
    ]
    total = jax.ShapeDtypeStruct((features, cols), f32)
    return pl.pallas_call(
        functools.partial(pair_kernel, n_tp),
        out_shape=(total, total, total, jax.ShapeDtypeStruct((model // LANES, LANES), f32)),
        in_specs=[pl.BlockSpec(memory_space=pltpu.HBM)] * 6,
        out_specs=(pl.BlockSpec(memory_space=pltpu.VMEM),) * 4,
        scratch_shapes=[pltpu.VMEM(shape, dtype) for shape, dtype in buffers] + [
            dma((7,)), dma((2,)), dma((2,)), dma((chunks,)), dma((chunks,)), dma((chunks, 2)), dma((chunks, 2)),
        ] + [dma((5, n_z))] * 6 + [dma((4,)), dma((4,)), pltpu.SemaphoreType.REGULAR, pltpu.VMEM((LANES, cols), f32)],
        compiler_params=pltpu.CompilerParams(
            collective_id=layer, has_side_effects=True, vmem_limit_bytes=VMEM_LIMIT,
        ),
    )(x, g, a, b, m, v)


def shards(n_dp, n_tp, proj_in, kv_grad, normed, norm_grad, first_moment, second_moment):
    layers, tokens, features = proj_in.shape
    rows, width = kv_grad.shape[1:]
    model = normed.shape[2]
    cols = width // n_dp
    lines = 8
    dma = pltpu.SemaphoreType.DMA
    n_z = n_tp // 2
    firsts, seconds, updates, gains = [], [], [], []
    for layer in range(layers):
        if n_dp == 4 and features % LANES == 0 and features >= 8 * LANES and model % (16 * LANES) == 0 and n_tp >= 6:
            new_first, new_second, update, gain = store_call(*pair_call(
                layer, n_tp, proj_in[layer], pltpu.with_memory_space_constraint(kv_grad[layer], pltpu.HBM), normed[layer], norm_grad[layer],
                first_moment[layer], second_moment[layer],
            ))
        else:
            total, gain = pl.pallas_call(
                functools.partial(kernel, n_dp, n_tp),
                out_shape=(
                    jax.ShapeDtypeStruct((features, cols), jnp.float32),
                    jax.ShapeDtypeStruct((lines, model // lines), jnp.float32),
                ),
                in_specs=[pl.BlockSpec(memory_space=pltpu.HBM)] * 4,
                out_specs=(pl.BlockSpec(memory_space=pltpu.VMEM), pl.BlockSpec(memory_space=pltpu.VMEM)),
                scratch_shapes=[
                    pltpu.VMEM((n_dp, tokens, features), jnp.bfloat16),
                    pltpu.VMEM((n_dp, n_tp * rows, cols), jnp.bfloat16),
                    pltpu.VMEM((rows, model), jnp.bfloat16),
                    pltpu.VMEM((rows, model), jnp.bfloat16),
                    pltpu.VMEM((n_tp, lines, model // lines), jnp.float32),
                    pltpu.VMEM((n_dp, lines, model // lines), jnp.float32),
                    dma((4,)),
                    dma((n_dp, PIECES)), dma((n_dp, PIECES)),
                    dma((n_dp,)), dma((n_dp,)),
                    dma((n_z,)), dma((n_z,)), dma((n_z,)), dma((n_z,)),
                    dma((n_z,)), dma((n_z,)),
                    dma((n_tp,)), dma((n_tp,)), dma((n_dp,)), dma((n_dp,)),
                ],
                compiler_params=pltpu.CompilerParams(
                    collective_id=layer, has_side_effects=True, vmem_limit_bytes=60 * 1024 * 1024,
                ),
            )(proj_in[layer], kv_grad[layer], normed[layer], norm_grad[layer])
            new_first, new_second, update = adam_update(total / n_dp, first_moment[layer], second_moment[layer])
        firsts.append(new_first)
        seconds.append(new_second)
        updates.append(update)
        gains.append(gain.reshape(model))
    return (jnp.stack(firsts), jnp.stack(seconds), jnp.stack(updates), jnp.stack(gains))


def solution(mesh):
    return jax.shard_map(
        functools.partial(shards, mesh.shape["dp"], mesh.shape["tp"]),
        mesh=mesh,
        in_specs=(
            P(None, "dp", "tp"),
            P(None, ("dp", "tp"), None),
            P(None, ("dp", "tp"), None),
            P(None, ("dp", "tp"), None),
            P(None, "tp", "dp"),
            P(None, "tp", "dp"),
        ),
        out_specs=(P(None, "tp", "dp"), P(None, "tp", "dp"), P(None, "tp", "dp"), P()),
        check_vma=False,
    )
```
